32 devices in a mesh: dp: 1 (over z), pool: 4 (over y), ep: 8 (over x, core).
Axes of the slice: x: 4, y: 4, z: 1, core: 2. Of those that a mesh axis runs over, the one named last changes fastest.
The devices are a block of a 4x4x8 slice.
Arguments:
- hidden: bfloat16 [4096, 1024], P(('dp', 'pool', 'ep'))
- k_cache: bfloat16 [2, 4096, 128, 1, 128], P(None, ('dp', 'pool', 'ep'))
- v_cache: bfloat16 [2, 4096, 128, 1, 128], P(None, ('dp', 'pool', 'ep'))
- lengths: int32 [4096], P(('dp', 'pool', 'ep'))
- w_query: bfloat16 [2, 1024, 2048], replicated
- w_key: bfloat16 [2, 1024, 128], replicated
- w_value: bfloat16 [2, 1024, 128], replicated
- w_out: bfloat16 [2, 2048, 1024], replicated
- w_router: float32 [2, 1024, 128], replicated
- expert_ids: int32 [2, 4096, 8], P(None, ('dp', 'pool', 'ep'))
- w_gate: bfloat16 [2, 128, 1024, 384], P(None, ('pool', 'ep'))
- w_up: bfloat16 [2, 128, 1024, 384], P(None, ('pool', 'ep'))
- w_down: bfloat16 [2, 128, 384, 1024], P(None, ('pool', 'ep'))
Outputs:
- output: bfloat16 [4096, 1024], P(('dp', 'pool', 'ep'))
All inputs are finite; a program needn't handle non-finite values.
Results may differ from the reference program's by a relative error of at most 0.02.
Values are sent between devices in bfloat16 or wider.
A program may use at most 768 MiB of HBM per device.

```python
import jax
import jax.numpy as jnp
from jax import lax

D = 1024
HEADS = 16
KV_HEADS = 1
HEAD = 128
EXPERTS = 128
TOP = 8
FF = 384
TOK_DEV = 128
SEQ_LEN = 128
GROUP = 32
LAYERS = 2
ATT_BLOCK = 8

TOKENS = GROUP * TOK_DEV
LOCAL_EXPERTS = EXPERTS // GROUP
PAIR_MEAN = TOK_DEV * TOP // GROUP
LINK_CAP = 2 * PAIR_MEAN - 1
EXPERT_CAP = GROUP * ((LINK_CAP + LOCAL_EXPERTS - 1) // LOCAL_EXPERTS)
PER_KV = HEADS // KV_HEADS
EPS = 1e-6
ATTN_SCALE = HEAD ** -0.5


def source_routing(counts, rng_key):
    flat_ids = jnp.repeat(jnp.arange(EXPERTS, dtype=jnp.int32), counts, total_repeat_length=TOK_DEV * TOP)
    laid_out = flat_ids.reshape(TOP, TOK_DEV).T
    return laid_out[jax.random.permutation(rng_key, TOK_DEV)]


def layer_routing(rng_key):
    order_key, spread_key, offset_key, token_key = jax.random.split(rng_key, 4)
    half_group = GROUP // 2
    device_order = jax.random.permutation(order_key, GROUP)
    hot_dev = device_order[:half_group]
    cold_dev = device_order[half_group:]
    spread = jax.random.randint(spread_key, (GROUP, half_group), 0, PAIR_MEAN)
    spread = spread.at[:, 0].set(PAIR_MEAN - 1)
    link_count = jnp.zeros((GROUP, GROUP), jnp.int32)
    link_count = link_count.at[:, hot_dev].set(PAIR_MEAN + spread)
    link_count = link_count.at[:, cold_dev].set(PAIR_MEAN - spread)
    offsets = jax.random.randint(offset_key, (GROUP, GROUP), 0, LOCAL_EXPERTS)
    offsets = offsets.at[:, hot_dev[0]].set(0)
    local_idx = jnp.arange(LOCAL_EXPERTS)
    extra_one = ((local_idx[None, None, :] - offsets[:, :, None]) % LOCAL_EXPERTS) < (link_count % LOCAL_EXPERTS)[:, :, None]
    expert_count = (link_count // LOCAL_EXPERTS)[:, :, None] + extra_one.astype(jnp.int32)
    token_keys = jax.random.split(token_key, GROUP)
    routed = jax.vmap(source_routing)(expert_count.reshape(GROUP, EXPERTS), token_keys)
    return routed.reshape(TOKENS, TOP)


def draw_lengths(rng_key):
    lengths = jax.random.randint(rng_key, (TOKENS,), SEQ_LEN // 2, SEQ_LEN + 1)
    return lengths.at[0].set(SEQ_LEN).at[1].set(SEQ_LEN // 2)


def setup_inputs(seed: int = 0, part: int = 0) -> dict:
    base_key = jax.random.key(seed)
    shared_keys = jax.random.split(base_key, 8)
    part_keys = jax.random.split(jax.random.fold_in(base_key, part), 5)
    cache_shape = (LAYERS, TOKENS, SEQ_LEN, KV_HEADS, HEAD)
    hidden = jax.random.normal(part_keys[0], (TOKENS, D), jnp.float32).astype(jnp.bfloat16)
    k_cache = jax.random.normal(part_keys[1], cache_shape, jnp.float32).astype(jnp.bfloat16)
    v_cache = jax.random.normal(part_keys[2], cache_shape, jnp.float32).astype(jnp.bfloat16)
    lengths = draw_lengths(part_keys[3])
    expert_ids = jax.vmap(layer_routing)(jax.random.split(part_keys[4], LAYERS))
    w_query = (jax.random.normal(shared_keys[0], (LAYERS, D, HEADS * HEAD), jnp.float32) * D ** -0.5).astype(jnp.bfloat16)
    w_key = (jax.random.normal(shared_keys[1], (LAYERS, D, KV_HEADS * HEAD), jnp.float32) * D ** -0.5).astype(jnp.bfloat16)
    w_value = (jax.random.normal(shared_keys[2], (LAYERS, D, KV_HEADS * HEAD), jnp.float32) * D ** -0.5).astype(jnp.bfloat16)
    w_out = (jax.random.normal(shared_keys[3], (LAYERS, HEADS * HEAD, D), jnp.float32) * (0.4 * (SEQ_LEN / (HEADS * HEAD)) ** 0.5)).astype(jnp.bfloat16)
    w_router = jax.random.normal(shared_keys[4], (LAYERS, D, EXPERTS), jnp.float32) * (1.5 * D ** -0.5)
    w_gate = (jax.random.normal(shared_keys[5], (LAYERS, EXPERTS, D, FF), jnp.float32) * D ** -0.5).astype(jnp.bfloat16)
    w_up = (jax.random.normal(shared_keys[6], (LAYERS, EXPERTS, D, FF), jnp.float32) * D ** -0.5).astype(jnp.bfloat16)
    w_down = (jax.random.normal(shared_keys[7], (LAYERS, EXPERTS, FF, D), jnp.float32) * (TOP / FF) ** 0.5).astype(jnp.bfloat16)
    return {"hidden": hidden, "k_cache": k_cache, "v_cache": v_cache, "lengths": lengths, "w_query": w_query, "w_key": w_key, "w_value": w_value, "w_out": w_out, "w_router": w_router, "expert_ids": expert_ids, "w_gate": w_gate, "w_up": w_up, "w_down": w_down}


def rms_norm(values):
    wide = values.astype(jnp.float32)
    inv_norm = lax.rsqrt(jnp.mean(wide * wide, axis=-1, keepdims=True) + EPS)
    return (wide * inv_norm).astype(jnp.bfloat16)


def attend_block(block):
    query, keys_blk, values_blk, len_blk, key_new, value_new = block
    query = query.astype(jnp.float32)
    scores = jnp.einsum('tkgd,tskd->tkgs', query, keys_blk.astype(jnp.float32)) * ATTN_SCALE
    valid_pos = jnp.arange(SEQ_LEN)[None, :] < len_blk[:, None]
    scores = jnp.where(valid_pos[:, None, None, :], scores, -jnp.inf)
    score_new = jnp.einsum('tkgd,tkd->tkg', query, key_new.astype(jnp.float32)) * ATTN_SCALE
    peak_score = jnp.maximum(jnp.max(scores, axis=-1), score_new)
    att_probs = jnp.exp(scores - peak_score[..., None])
    new_prob = jnp.exp(score_new - peak_score)
    norm_total = jnp.sum(att_probs, axis=-1) + new_prob
    att_probs = (att_probs / norm_total[..., None]).astype(jnp.bfloat16)
    new_prob = (new_prob / norm_total).astype(jnp.bfloat16)
    mixed = jnp.einsum('tkgs,tskd->tkgd', att_probs.astype(jnp.float32), values_blk.astype(jnp.float32))
    mixed = mixed + new_prob.astype(jnp.float32)[..., None] * value_new.astype(jnp.float32)[:, :, None, :]
    return mixed.astype(jnp.bfloat16)


def expert_mix(routed, layer_ids, gates, g_weight, u_weight, d_weight):
    flat_ids = layer_ids.reshape(-1)
    pair_count = TOKENS * TOP
    sort_order = jnp.argsort(flat_ids, stable=True)
    sorted_ids = flat_ids[sort_order]
    counts = jnp.bincount(flat_ids, length=EXPERTS)
    starts = jnp.cumsum(counts) - counts
    ranks = jnp.arange(pair_count) - starts[sorted_ids]
    pair_for_slot = jnp.full((EXPERTS * EXPERT_CAP,), pair_count, jnp.int32)
    pair_for_slot = pair_for_slot.at[sorted_ids * EXPERT_CAP + ranks].set(sort_order.astype(jnp.int32), mode='drop')
    flat_gates = gates.reshape(-1)

    def expert_body(carry, item):
        gate_w, up_w, down_w, pair_idx = item
        token_idx = pair_idx // TOP
        rows = jnp.take(routed, token_idx, axis=0, mode='fill', fill_value=0)
        first = jnp.dot(rows, gate_w, preferred_element_type=jnp.float32)
        second = jnp.dot(rows, up_w, preferred_element_type=jnp.float32)
        inner = (jax.nn.silu(first) * second).astype(jnp.bfloat16)
        out_rows = jnp.dot(inner, down_w, preferred_element_type=jnp.float32).astype(jnp.bfloat16)
        weight = jnp.take(flat_gates, pair_idx, mode='fill', fill_value=0)
        carry = carry.at[token_idx].add(weight[:, None] * out_rows.astype(jnp.float32), mode='drop')
        return carry, None

    windows = pair_for_slot.reshape(EXPERTS, EXPERT_CAP)
    return lax.scan(expert_body, jnp.zeros((TOKENS, D), jnp.float32), (g_weight, u_weight, d_weight, windows))[0]


def reference(hidden, k_cache, v_cache, lengths, w_query, w_key, w_value, w_out, w_router, expert_ids, w_gate, w_up, w_down):
    blocks = TOKENS // ATT_BLOCK

    def layer_step(state, layer):
        cache_k, cache_v, q_weight, k_weight, v_weight, o_weight, r_weight, layer_ids, g_weight, u_weight, d_weight = layer
        normed = rms_norm(state)
        query = jnp.dot(normed, q_weight, preferred_element_type=jnp.float32).astype(jnp.bfloat16)
        key_new = jnp.dot(normed, k_weight, preferred_element_type=jnp.float32).astype(jnp.bfloat16)
        value_new = jnp.dot(normed, v_weight, preferred_element_type=jnp.float32).astype(jnp.bfloat16)
        mixed = lax.map(attend_block, (
            query.reshape(blocks, ATT_BLOCK, KV_HEADS, PER_KV, HEAD),
            cache_k.reshape(blocks, ATT_BLOCK, SEQ_LEN, KV_HEADS, HEAD),
            cache_v.reshape(blocks, ATT_BLOCK, SEQ_LEN, KV_HEADS, HEAD),
            lengths.reshape(blocks, ATT_BLOCK),
            key_new.reshape(blocks, ATT_BLOCK, KV_HEADS, HEAD),
            value_new.reshape(blocks, ATT_BLOCK, KV_HEADS, HEAD)))
        mixed = mixed.reshape(TOKENS, HEADS * HEAD)
        residual = (state.astype(jnp.float32) + jnp.dot(mixed, o_weight, preferred_element_type=jnp.float32)).astype(jnp.bfloat16)
        routed = rms_norm(residual)
        logits = jnp.dot(routed.astype(jnp.float32), r_weight, preferred_element_type=jnp.float32)
        gates = jax.nn.softmax(jnp.take_along_axis(logits, layer_ids, axis=1), axis=-1)
        combined = expert_mix(routed, layer_ids, gates, g_weight, u_weight, d_weight)
        return (residual.astype(jnp.float32) + combined).astype(jnp.bfloat16), None

    layer_inputs = (k_cache, v_cache, w_query, w_key, w_value, w_out, w_router, expert_ids, w_gate, w_up, w_down)
    return lax.scan(layer_step, hidden, layer_inputs)[0]
```

```python
import functools

import jax
import jax.numpy as jnp
from jax import lax
from jax.experimental import pallas as pl
from jax.experimental.pallas import tpu as pltpu
from jax.sharding import PartitionSpec as P

EPS = 1e-6
GROUP_AXES = ('pool', 'ep')
BATCH_AXES = ('dp', 'pool', 'ep')
F32 = jnp.float32
BF16 = jnp.bfloat16
CHUNK = 16
WINDOW = 64
TILE = 256
VMEM_LIMIT = 60 * 1024 * 1024


def rms_norm(wide):
    return (wide * lax.rsqrt(jnp.mean(wide * wide, axis=-1, keepdims=True) + EPS)).astype(BF16)


def dot(a, b):
    return jnp.dot(a, b, preferred_element_type=F32)


def dot_t(a, b):
    return lax.dot_general(a, b, (((1,), (1,)), ((), ())), preferred_element_type=F32)


def split3(w):
    hi = w.astype(BF16)
    rest = w - hi.astype(F32)
    mid = rest.astype(BF16)
    low = (rest - mid.astype(F32)).astype(BF16)
    return hi, mid, low


def attention_kernel(layer, dims, hidden_ref, kc_hbm, vc_hbm, len_ref, wq_hbm, wk_hbm, wv_hbm, wo_hbm, wr_hbm, ids_ref,
                     a_ref, u_ref, gate_ref, slot_ref,
                     kbuf, vbuf, wq, wk, wv, wo, wr, q3, o3, kn3, vn3, ksem, vsem, wsem):
    tok, heads, hd, seq, experts, local, top, blk = dims
    nblk = tok // blk
    w_copies = [pltpu.make_async_copy(src.at[layer], dst, wsem.at[i])
                for i, (src, dst) in enumerate(((wq_hbm, wq), (wk_hbm, wk), (wv_hbm, wv), (wo_hbm, wo), (wr_hbm, wr)))]
    for cp in w_copies[:3]:
        cp.start()

    def kv_copy(b):
        rows = pl.ds(b * blk, blk)
        return (pltpu.make_async_copy(kc_hbm.at[layer, rows], kbuf.at[rows], ksem.at[b]),
                pltpu.make_async_copy(vc_hbm.at[layer, rows], vbuf.at[rows], vsem.at[b]))

    for b in range(nblk):
        kcp, vcp = kv_copy(b)
        kcp.start()
        vcp.start()
    for cp in w_copies[3:]:
        cp.start()

    hidden = hidden_ref[...].astype(F32)
    normed = rms_norm(hidden)
    for cp in w_copies[:3]:
        cp.wait()
    kn3[...] = dot(normed, wk[...]).astype(BF16).astype(F32)
    vn3[...] = dot(normed, wv[...]).astype(BF16).astype(F32)
    for h in range(heads):
        if h % 2 == 0:
            pair = dot(normed, wq[:, h * hd:(h + 2) * hd])
        q3[:, h, :] = pair[:, (h % 2) * hd:(h % 2 + 1) * hd].astype(BF16).astype(F32)

    scale = hd ** -0.5
    lane = lax.broadcasted_iota(jnp.int32, (heads, seq), 1)

    def block(b, carry):
        kcp, vcp = kv_copy(b)
        kcp.wait()
        vcp.wait()
        for j in range(blk):
            t = b * blk + j
            q = q3[t]
            s = dot_t(q.astype(BF16), kbuf[t]) * scale
            s = jnp.where(lane < len_ref[t], s, -jnp.inf)
            sn = jnp.sum(q * kn3[pl.ds(t, 1), :], axis=1, keepdims=True) * scale
            peak = jnp.maximum(jnp.max(s, axis=1, keepdims=True), sn)
            p = jnp.exp(s - peak)
            pn = jnp.exp(sn - peak)
            inv = 1.0 / (jnp.sum(p, axis=1, keepdims=True) + pn)
            pb = (p * inv).astype(BF16)
            pnb = (pn * inv).astype(BF16).astype(F32)
            o = dot(pb, vbuf[t]) + pnb * vn3[pl.ds(t, 1), :]
            o3[t] = o.astype(BF16).astype(F32)
        return carry

    lax.fori_loop(0, nblk, block, 0)

    for cp in w_copies[3:]:
        cp.wait()
    mixed = jnp.concatenate([o3[:, h, :].astype(BF16) for h in range(heads)], axis=1)
    a = (hidden + dot(mixed, wo[...])).astype(BF16)
    a_ref[...] = a
    u = rms_norm(a.astype(F32))
    u_ref[...] = u
    hi, mid, low = split3(wr[...])
    logits = dot(u, hi) + dot(u, mid) + dot(u, low)

    ids = ids_ref[...]
    e_iota = lax.broadcasted_iota(jnp.int32, (tok, experts), 1)
    t_row = lax.broadcasted_iota(jnp.int32, (tok, tok), 0)
    t_col = lax.broadcasted_iota(jnp.int32, (tok, tok), 1)
    before = jnp.where(t_col < t_row, 1.0, 0.0).astype(BF16)
    e_row = lax.broadcasted_iota(jnp.int32, (experts, experts), 0)
    e_col = lax.broadcasted_iota(jnp.int32, (experts, experts), 1)
    same = jnp.where((e_row < e_col) & (e_row // local == e_col // local), 1.0, 0.0).astype(BF16)
    hits = [ids[:, k:k + 1] == e_iota for k in range(top)]
    chosen = hits[0]
    for k in range(1, top):
        chosen = chosen | hits[k]
    chosen = jnp.where(chosen, 1.0, 0.0)
    rank = dot(before, chosen.astype(BF16))
    count = jnp.sum(chosen, axis=0, keepdims=True)
    start = dot(jnp.broadcast_to(count, (8, experts)).astype(BF16), same)[0:1]
    slot_full = rank + start + ((e_iota // local) * WINDOW).astype(F32)
    picked = [jnp.sum(jnp.where(hits[k], logits, 0.0), axis=1, keepdims=True) for k in range(top)]
    peak = picked[0]
    for k in range(1, top):
        peak = jnp.maximum(peak, picked[k])
    ex = [jnp.exp(v - peak) for v in picked]
    total = ex[0]
    for k in range(1, top):
        total = total + ex[k]
    for k in range(top):
        gate_ref[:, k:k + 1] = ex[k] / total
        slot_ref[:, k:k + 1] = jnp.sum(jnp.where(hits[k], slot_full, 0.0), axis=1, keepdims=True).astype(jnp.int32)


def attention(layer, hidden, k_cache, v_cache, lengths, w_query, w_key, w_value, w_out, w_router, ids, local):
    tok, width = hidden.shape
    seq, hd = k_cache.shape[2], k_cache.shape[3]
    heads = w_query.shape[2] // hd
    experts = w_router.shape[2]
    top = ids.shape[1]
    blk = 16
    dims = (tok, heads, hd, seq, experts, local, top, blk)
    vm = pl.BlockSpec(memory_space=pltpu.VMEM)
    hb = pl.BlockSpec(memory_space=pl.ANY)
    sm = pl.BlockSpec(memory_space=pltpu.SMEM)
    return pl.pallas_call(
        functools.partial(attention_kernel, layer, dims),
        out_shape=(jax.ShapeDtypeStruct((tok, width), BF16), jax.ShapeDtypeStruct((tok, width), BF16),
                   jax.ShapeDtypeStruct((tok, top), F32), jax.ShapeDtypeStruct((tok, top), jnp.int32)),
        in_specs=[vm, hb, hb, sm, hb, hb, hb, hb, hb, vm],
        out_specs=(vm, vm, vm, vm),
        scratch_shapes=[
            pltpu.VMEM((tok, seq, hd), BF16), pltpu.VMEM((tok, seq, hd), BF16),
            pltpu.VMEM((width, heads * hd), BF16), pltpu.VMEM((width, hd), BF16), pltpu.VMEM((width, hd), BF16),
            pltpu.VMEM((heads * hd, width), BF16), pltpu.VMEM((width, experts), F32),
            pltpu.VMEM((tok, heads, hd), F32), pltpu.VMEM((tok, heads, hd), F32),
            pltpu.VMEM((tok, hd), F32), pltpu.VMEM((tok, hd), F32),
            pltpu.SemaphoreType.DMA((tok // blk,)), pltpu.SemaphoreType.DMA((tok // blk,)), pltpu.SemaphoreType.DMA((5,)),
        ],
        compiler_params=pltpu.CompilerParams(vmem_limit_bytes=VMEM_LIMIT),
        cost_estimate=pl.CostEstimate(flops=4 * 10 ** 9, bytes_accessed=20 * 10 ** 6, transcendentals=0),
        name='attention',
    )(hidden, k_cache, v_cache, lengths, w_query, w_key, w_value, w_out, w_router, ids)


def tables_kernel(dims, ids_ref, key_ref, cnt_ref):
    layers, group, top, tok, local = dims
    me = lax.axis_index(GROUP_AXES)
    row = lax.broadcasted_iota(jnp.int32, (tok, tok), 0)
    col = lax.broadcasted_iota(jnp.int32, (tok, tok), 1)
    before = jnp.where(row < col, 1.0, 0.0).astype(BF16)
    ones = jnp.ones((8, tok), BF16)
    for layer in range(layers):
        for e in range(local):
            target = me * local + e
            hit = ids_ref[:, layer * top, :] == target
            for k in range(1, top):
                hit = hit | (ids_ref[:, layer * top + k, :] == target)
            hitb = jnp.where(hit, 1.0, 0.0).astype(BF16)
            key_ref[layer * local + e] = jnp.where(hit, dot(hitb, before).astype(jnp.int32), -1024)
            cnt_ref[layer * local + e:layer * local + e + 1, :] = dot_t(ones, hitb)[0:1].astype(jnp.int32)


def tables(ids_all, layers, top, local):
    group, _, tok = ids_all.shape
    vm = pl.BlockSpec(memory_space=pltpu.VMEM)
    return pl.pallas_call(
        functools.partial(tables_kernel, (layers, group, top, tok, local)),
        out_shape=(jax.ShapeDtypeStruct((layers * local, group, tok), jnp.int32),
                   jax.ShapeDtypeStruct((layers * local, group), jnp.int32)),
        in_specs=[vm], out_specs=(vm, vm), name='tables',
    )(ids_all)


def expert_kernel(layer, dims, u_hbm, key_ref, cnt_ref, wg_hbm, wu_hbm, wd_hbm, r_ref,
                  ubuf, xg, xs, ys, yc, wg, wu, wd, tab, usem, wsem):
    pools, tok, local, cap_chunks, pool_chunks = dims
    pool_rows = pool_chunks * CHUNK

    def u_copy(c):
        return pltpu.make_async_copy(u_hbm.at[c], ubuf.at[c], usem.at[c])

    def w_copies(e):
        return [pltpu.make_async_copy(src.at[layer, e], dst.at[e], wsem.at[i, e])
                for i, (src, dst) in enumerate(((wg_hbm, wg), (wu_hbm, wu), (wd_hbm, wd)))]

    for c in range(pools):
        u_copy(c).start()
    for e in range(local):
        for cp in w_copies(e):
            cp.start()

    ys[0] = jnp.zeros(ys.shape[1:], BF16)
    row = lax.broadcasted_iota(jnp.int32, (pool_rows, tok), 0)

    def counts(c):
        even = [cnt_ref[layer * local + e, 2 * c] for e in range(local)]
        odd = [cnt_ref[layer * local + e, 2 * c + 1] for e in range(local)]
        chunks = [(even[e] + odd[e] + (CHUNK - 1)) // CHUNK for e in range(local)]
        return even, odd, chunks

    def gather(c, base):
        u_copy(c).wait()
        even, odd, chunks = counts(c)
        halves = []
        for par in range(2):
            off = jnp.int32(0)
            hit = None
            for e in range(local):
                shift = off * CHUNK + (even[e] if par else 0)
                this = row == key_ref[layer * local + e, pl.ds(2 * c + par, 1), :] + shift
                hit = this if hit is None else hit | this
                off = off + chunks[e]
            halves.append(jnp.where(hit, 1.0, 0.0).astype(BF16))
        pick = jnp.concatenate(halves, axis=1)
        xg[...] = dot(pick, ubuf[c]).astype(BF16).reshape(xg.shape)
        for i in range(pool_chunks):
            tab[c * pool_chunks + i] = 0
        off = jnp.int32(0)
        new_base = []
        for e in range(local):
            def copy(i, carry, e=e, off=off):
                to = e * cap_chunks + base[e] + i
                xs[to] = xg[off + i]
                tab[c * pool_chunks + off + i] = to
                return carry
            lax.fori_loop(0, chunks[e], copy, 0)
            off = off + chunks[e]
            new_base.append(base[e] + chunks[e])
        return tuple(new_base)

    base = lax.fori_loop(0, pools, gather, tuple(jnp.int32(0) for _ in range(local)))

    per = TILE // CHUNK
    for e in range(local):
        for cp in w_copies(e):
            cp.wait()

        def tile(i, carry, e=e):
            at = pl.ds(e * cap_chunks + i * per, per)
            x = xs[at].reshape(TILE, xs.shape[2])
            first = dot(x, wg[e])
            second = dot(x, wu[e])
            inner = (first * (1.0 / (1.0 + jnp.exp(-first))) * second).astype(BF16)
            ys[at] = dot(inner, wd[e]).astype(BF16).reshape(per, CHUNK, xs.shape[2])
            return carry

        lax.fori_loop(0, (base[e] + per - 1) // per, tile, 0)

    jrow = lax.broadcasted_iota(jnp.int32, (WINDOW, pool_rows), 0)
    diff = lax.broadcasted_iota(jnp.int32, (WINDOW, pool_rows), 1) - jrow

    def give_back(c, carry):
        even, odd, chunks = counts(c)
        for i in range(pool_chunks):
            yc[i] = ys[tab[c * pool_chunks + i]]
        halves = []
        for par in range(2):
            off = jnp.int32(0)
            lo = jnp.int32(0)
            hit = None
            for e in range(local):
                n = odd[e] if par else even[e]
                delta = off * CHUNK + (even[e] if par else 0) - lo
                this = (diff == delta) & (jrow >= lo) & (jrow < lo + n)
                hit = this if hit is None else hit | this
                off = off + chunks[e]
                lo = lo + n
            halves.append(jnp.where(hit, 1.0, 0.0).astype(BF16))
        pick = jnp.concatenate(halves, axis=0)
        r_ref[pl.ds(2 * c, 2)] = dot(pick, yc[...].reshape(pool_rows, yc.shape[2])).astype(BF16).reshape(2, WINDOW, yc.shape[2])
        return carry

    lax.fori_loop(0, pools, give_back, 0)


def experts(layer, u_all, keys, cnt, w_gate, w_up, w_down):
    group, tok, width = u_all.shape
    pools = group // 2
    local, ff = w_gate.shape[1], w_gate.shape[3]
    pool_chunks = (2 * (WINDOW - 1) + local * (CHUNK - 1) + CHUNK - 1) // CHUNK
    cap = pl.cdiv(group * CHUNK + pools * (CHUNK - 1), TILE) * TILE
    cap_chunks = cap // CHUNK
    u_pool = u_all.reshape(pools, 2 * tok, width)
    vm = pl.BlockSpec(memory_space=pltpu.VMEM)
    hb = pl.BlockSpec(memory_space=pl.ANY)
    sm = pl.BlockSpec(memory_space=pltpu.SMEM)
    return pl.pallas_call(
        functools.partial(expert_kernel, layer, (pools, tok, local, cap_chunks, pool_chunks)),
        out_shape=jax.ShapeDtypeStruct((group, WINDOW, width), BF16),
        in_specs=[hb, vm, sm, hb, hb, hb],
        out_specs=vm,
        scratch_shapes=[
            pltpu.VMEM((pools, 2 * tok, width), BF16),
            pltpu.VMEM((pool_chunks, CHUNK, width), BF16),
            pltpu.VMEM((local * cap_chunks, CHUNK, width), BF16),
            pltpu.VMEM((local * cap_chunks, CHUNK, width), BF16),
            pltpu.VMEM((pool_chunks, CHUNK, width), BF16),
            pltpu.VMEM((local, width, ff), BF16), pltpu.VMEM((local, width, ff), BF16), pltpu.VMEM((local, ff, width), BF16),
            pltpu.SMEM((pools * pool_chunks,), jnp.int32),
            pltpu.SemaphoreType.DMA((pools,)), pltpu.SemaphoreType.DMA((3, local)),
        ],
        compiler_params=pltpu.CompilerParams(vmem_limit_bytes=VMEM_LIMIT),
        cost_estimate=pl.CostEstimate(flops=6 * 10 ** 9, bytes_accessed=20 * 10 ** 6, transcendentals=0),
        name='experts',
    )(u_pool, keys, cnt, w_gate, w_up, w_down)


def combine_kernel(a_ref, r_ref, gate_ref, slot_ref, x_ref, gmat):
    tok, top = gate_ref.shape
    slots = r_ref.shape[0]
    step = 512
    for j in range(0, slots, step):
        iota = lax.broadcasted_iota(jnp.int32, (tok, step), 1) + j
        g = jnp.zeros((tok, step), F32)
        for k in range(top):
            g = jnp.where(iota == slot_ref[:, k:k + 1], gate_ref[:, k:k + 1], g)
        hi, mid, low = split3(g)
        gmat[0:tok, j:j + step] = hi
        gmat[tok:2 * tok, j:j + step] = mid
        gmat[2 * tok:3 * tok, j:j + step] = low
    width = x_ref.shape[1]
    half = width // 2
    for n in range(0, width, half):
        parts = dot(gmat[...], r_ref[:, n:n + half])
        total = parts[0:tok] + parts[tok:2 * tok] + parts[2 * tok:3 * tok]
        x_ref[:, n:n + half] = (a_ref[:, n:n + half].astype(F32) + total).astype(BF16)


def combine(a, rows, gates, slots):
    tok, width = a.shape
    vm = pl.BlockSpec(memory_space=pltpu.VMEM)
    return pl.pallas_call(
        combine_kernel,
        out_shape=jax.ShapeDtypeStruct((tok, width), BF16),
        in_specs=[vm] * 4, out_specs=vm,
        scratch_shapes=[pltpu.VMEM((3 * tok, rows.shape[0]), BF16)],
        compiler_params=pltpu.CompilerParams(vmem_limit_bytes=VMEM_LIMIT),
        name='combine',
    )(a, rows, gates, slots)


def solution(mesh):
    def device_step(hidden, k_cache, v_cache, lengths, w_query, w_key, w_value, w_out, w_router, expert_ids, w_gate, w_up, w_down):
        tok, width = hidden.shape
        layers, _, top = expert_ids.shape
        local = w_gate.shape[1]
        k_cache = k_cache.reshape(layers, tok, k_cache.shape[2], k_cache.shape[4])
        v_cache = v_cache.reshape(k_cache.shape)
        ids_all = lax.all_gather(jnp.swapaxes(expert_ids, 1, 2).reshape(layers * top, tok), GROUP_AXES, axis=0)
        keys, cnt = tables(ids_all, layers, top, local)
        for layer in range(layers):
            a, u, gates, slots = attention(layer, hidden, k_cache, v_cache, lengths, w_query, w_key, w_value, w_out, w_router, expert_ids[layer], local)
            u_all = lax.all_gather(u, GROUP_AXES, axis=0)
            rows = experts(layer, u_all, keys, cnt, w_gate, w_up, w_down)
            back = lax.all_to_all(rows, GROUP_AXES, 0, 0, tiled=True)
            hidden = combine(a, back.reshape(-1, width), gates, slots)
        return hidden

    cache_spec = P(None, BATCH_AXES, None, None, None)
    expert_spec = P(None, GROUP_AXES, None, None)
    in_specs = (P(BATCH_AXES, None), cache_spec, cache_spec, P(BATCH_AXES), P(), P(), P(), P(), P(), P(None, BATCH_AXES, None), expert_spec, expert_spec, expert_spec)
    return jax.shard_map(device_step, mesh=mesh, in_specs=in_specs, out_specs=P(BATCH_AXES, None), check_vma=False)
```

```python
import functools

import jax
import jax.numpy as jnp
from jax import lax
from jax.experimental import pallas as pl
from jax.experimental.pallas import tpu as pltpu
from jax.sharding import PartitionSpec as P

EPS = 1e-6
GROUP_AXES = ('pool', 'ep')
BATCH_AXES = ('dp', 'pool', 'ep')
F32 = jnp.float32
BF16 = jnp.bfloat16
CHUNK = 16
WINDOW = 64
TILE = 256
VMEM_LIMIT = 60 * 1024 * 1024
MESH = pl.DeviceIdType.MESH


def rms_norm(wide):
    return (wide * lax.rsqrt(jnp.mean(wide * wide, axis=-1, keepdims=True) + EPS)).astype(BF16)


def dot(a, b):
    return jnp.dot(a, b, preferred_element_type=F32)


def dot_t(a, b):
    return lax.dot_general(a, b, (((1,), (1,)), ((), ())), preferred_element_type=F32)


def split3(w):
    hi = w.astype(BF16)
    rest = w - hi.astype(F32)
    mid = rest.astype(BF16)
    low = (rest - mid.astype(F32)).astype(BF16)
    return hi, mid, low


def attention_kernel(layer, dims, share, hidden_ref, kc_hbm, vc_hbm, len_ref, wq_hbm, wk_hbm, wv_hbm, wo_hbm, wr_hbm, ids_ref, *refs):
    if share:
        mine_ref, a_ref, u_ref, gs_ref, all_ref, gather_buf, id_send, id_recv, *refs = refs
    else:
        a_ref, u_ref, gs_ref, *refs = refs
    attention_body(layer, dims, hidden_ref, kc_hbm, vc_hbm, len_ref, wq_hbm, wk_hbm, wv_hbm, wo_hbm, wr_hbm, ids_ref, a_ref, u_ref, gs_ref,
                   (lambda: share_ids(share, mine_ref, gather_buf, id_send, id_recv)) if share else None, *refs)
    if share:
        group = share[0] * share[1]
        me = lax.axis_index(GROUP_AXES)
        for d in range(1, group):
            id_copy(share, d, mine_ref, gather_buf, id_send, id_recv).wait()
        gather_buf[me] = mine_ref[...]
        all_ref[...] = gather_buf[...]


def id_copy(share, d, mine_ref, gather_buf, id_send, id_recv):
    pools, eps = share
    me = lax.axis_index(GROUP_AXES)
    to = lax.rem(me + d, pools * eps)
    return pltpu.make_async_remote_copy(
        src_ref=mine_ref, dst_ref=gather_buf.at[me], send_sem=id_send.at[d], recv_sem=id_recv.at[d],
        device_id={'pool': to // eps, 'ep': lax.rem(to, eps)}, device_id_type=MESH)


def share_ids(share, mine_ref, gather_buf, id_send, id_recv):
    pools, eps = share
    group = pools * eps
    me = lax.axis_index(GROUP_AXES)
    barrier = pltpu.get_barrier_semaphore()
    for d in range(1, group):
        to = lax.rem(me + d, group)
        pl.semaphore_signal(barrier, inc=1, device_id={'pool': to // eps, 'ep': lax.rem(to, eps)}, device_id_type=MESH)
    pl.semaphore_wait(barrier, group - 1)
    for d in range(1, group):
        id_copy(share, d, mine_ref, gather_buf, id_send, id_recv).start()


def attention_body(layer, dims, hidden_ref, kc_hbm, vc_hbm, len_ref, wq_hbm, wk_hbm, wv_hbm, wo_hbm, wr_hbm, ids_ref,
                   a_ref, u_ref, gs_ref, after_start,
                   kbuf, vbuf, wq, wk, wv, wo, wr, q3, o3, sbuf, nbuf, kn3, vn3, ksem, vsem, wsem):
    tok, heads, hd, seq, experts, local, top, blk = dims
    nblk = tok // blk
    w_copies = [pltpu.make_async_copy(src.at[layer], dst, wsem.at[i])
                for i, (src, dst) in enumerate(((wq_hbm, wq), (wk_hbm, wk), (wv_hbm, wv), (wo_hbm, wo), (wr_hbm, wr)))]
    for cp in w_copies[:3]:
        cp.start()

    def kv_copy(b):
        rows = pl.ds(b * blk, blk)
        return (pltpu.make_async_copy(kc_hbm.at[layer, rows], kbuf.at[rows], ksem.at[b]),
                pltpu.make_async_copy(vc_hbm.at[layer, rows], vbuf.at[rows], vsem.at[b]))

    for b in range(nblk):
        kcp, vcp = kv_copy(b)
        kcp.start()
        vcp.start()
    for cp in w_copies[3:]:
        cp.start()

    if after_start is not None:
        after_start()
    hidden = hidden_ref[...].astype(F32)
    normed = rms_norm(hidden)
    for cp in w_copies[:3]:
        cp.wait()
    kn3[...] = dot(normed, wk[...]).astype(BF16).astype(F32)
    vn3[...] = dot(normed, wv[...]).astype(BF16).astype(F32)
    for h in range(heads):
        if h % 2 == 0:
            pair = dot(normed, wq[:, h * hd:(h + 2) * hd])
        q3[:, h, :] = pair[:, (h % 2) * hd:(h % 2 + 1) * hd].astype(BF16).astype(F32)

    scale = hd ** -0.5
    lane = lax.broadcasted_iota(jnp.int32, (heads, seq), 1)

    def block(b, carry):
        kcp, vcp = kv_copy(b)
        kcp.wait()
        for j in range(blk):
            t = b * blk + j
            q = q3[t]
            s = dot_t(q.astype(BF16), kbuf[t]) * scale
            sbuf[j * heads:(j + 1) * heads, :] = jnp.where(lane < len_ref[t], s, -jnp.inf)
            nbuf[j * heads:(j + 1) * heads, :] = q * kn3[pl.ds(t, 1), :]
        s = sbuf[...]
        sn = jnp.sum(nbuf[...], axis=1, keepdims=True) * scale
        peak = jnp.maximum(jnp.max(s, axis=1, keepdims=True), sn)
        p = jnp.exp(s - peak)
        pn = jnp.exp(sn - peak)
        inv = 1.0 / (jnp.sum(p, axis=1, keepdims=True) + pn)
        pb = (p * inv).astype(BF16)
        pnb = (pn * inv).astype(BF16).astype(F32)
        vcp.wait()
        for j in range(blk):
            t = b * blk + j
            rows = slice(j * heads, (j + 1) * heads)
            o = dot(pb[rows], vbuf[t]) + pnb[rows] * vn3[pl.ds(t, 1), :]
            o3[t] = o.astype(BF16).astype(F32)
        return carry

    lax.fori_loop(0, nblk, block, 0)

    for cp in w_copies[3:]:
        cp.wait()
    mixed = jnp.concatenate([o3[:, h, :].astype(BF16) for h in range(heads)], axis=1)
    a = (hidden + dot(mixed, wo[...])).astype(BF16)
    a_ref[...] = a
    u = rms_norm(a.astype(F32))
    u_ref[...] = u
    hi, mid, low = split3(wr[...])
    logits = dot(u, hi) + dot(u, mid) + dot(u, low)

    ids = ids_ref[...]
    e_iota = lax.broadcasted_iota(jnp.int32, (tok, experts), 1)
    t_row = lax.broadcasted_iota(jnp.int32, (tok, tok), 0)
    t_col = lax.broadcasted_iota(jnp.int32, (tok, tok), 1)
    before = jnp.where(t_col < t_row, 1.0, 0.0).astype(BF16)
    e_row = lax.broadcasted_iota(jnp.int32, (experts, experts), 0)
    e_col = lax.broadcasted_iota(jnp.int32, (experts, experts), 1)
    same = jnp.where((e_row < e_col) & (e_row // local == e_col // local), 1.0, 0.0).astype(BF16)
    hits = [ids[:, k:k + 1] == e_iota for k in range(top)]
    chosen = hits[0]
    for k in range(1, top):
        chosen = chosen | hits[k]
    chosen = jnp.where(chosen, 1.0, 0.0)
    rank = dot(before, chosen.astype(BF16))
    count = jnp.sum(chosen, axis=0, keepdims=True)
    start = dot(jnp.broadcast_to(count, (8, experts)).astype(BF16), same)[0:1]
    slot_full = rank + start + ((e_iota // local) * WINDOW).astype(F32)
    picked = [jnp.sum(jnp.where(hits[k], logits, 0.0), axis=1, keepdims=True) for k in range(top)]
    peak = picked[0]
    for k in range(1, top):
        peak = jnp.maximum(peak, picked[k])
    ex = [jnp.exp(v - peak) for v in picked]
    total = ex[0]
    for k in range(1, top):
        total = total + ex[k]
    columns = [v / total for v in ex] + [jnp.sum(jnp.where(hit, slot_full, 0.0), axis=1, keepdims=True) for hit in hits]
    columns.append(jnp.zeros((tok, experts - 2 * top), F32))
    gs_ref[...] = jnp.transpose(jnp.concatenate(columns, axis=1))[:2 * top]


def attention(layer, share, hidden, k_cache, v_cache, lengths, w_query, w_key, w_value, w_out, w_router, ids, mine, local):
    tok, width = hidden.shape
    seq, hd = k_cache.shape[2], k_cache.shape[3]
    heads = w_query.shape[2] // hd
    experts = w_router.shape[2]
    top = ids.shape[1]
    blk = 16
    dims = (tok, heads, hd, seq, experts, local, top, blk)
    vm = pl.BlockSpec(memory_space=pltpu.VMEM)
    hb = pl.BlockSpec(memory_space=pl.ANY)
    sm = pl.BlockSpec(memory_space=pltpu.SMEM)
    out_shape = [jax.ShapeDtypeStruct((tok, width), BF16), jax.ShapeDtypeStruct((tok, width), BF16), jax.ShapeDtypeStruct((2 * top, tok), F32)]
    args = [hidden, k_cache, v_cache, lengths, w_query, w_key, w_value, w_out, w_router, ids]
    specs = [vm, hb, hb, sm, hb, hb, hb, hb, hb, vm]
    scratch = []
    params = {}
    if share:
        group = share[0] * share[1]
        args.append(mine)
        specs.append(vm)
        out_shape.append(jax.ShapeDtypeStruct((group,) + mine.shape, mine.dtype))
        scratch = [pltpu.VMEM((group,) + mine.shape, mine.dtype), pltpu.SemaphoreType.DMA((group,)), pltpu.SemaphoreType.DMA((group,))]
        params = dict(collective_id=7, has_side_effects=True)
    return pl.pallas_call(
        functools.partial(attention_kernel, layer, dims, share),
        out_shape=tuple(out_shape),
        in_specs=specs,
        out_specs=tuple(vm for _ in out_shape),
        scratch_shapes=scratch + [
            pltpu.VMEM((tok, seq, hd), BF16), pltpu.VMEM((tok, seq, hd), BF16),
            pltpu.VMEM((width, heads * hd), BF16), pltpu.VMEM((width, hd), BF16), pltpu.VMEM((width, hd), BF16),
            pltpu.VMEM((heads * hd, width), BF16), pltpu.VMEM((width, experts), F32),
            pltpu.VMEM((tok, heads, hd), F32), pltpu.VMEM((tok, heads, hd), F32),
            pltpu.VMEM((blk * heads, seq), F32), pltpu.VMEM((blk * heads, hd), F32),
            pltpu.VMEM((tok, hd), F32), pltpu.VMEM((tok, hd), F32),
            pltpu.SemaphoreType.DMA((tok // blk,)), pltpu.SemaphoreType.DMA((tok // blk,)), pltpu.SemaphoreType.DMA((5,)),
        ],
        compiler_params=pltpu.CompilerParams(vmem_limit_bytes=VMEM_LIMIT, **params),
        cost_estimate=pl.CostEstimate(flops=4 * 10 ** 9, bytes_accessed=20 * 10 ** 6, transcendentals=0),
        name='attention',
    )(*args)


def tables_kernel(dims, ids_ref, key_ref, tab_ref):
    layers, group, top, tok, local, pool_chunks, cap_chunks = dims
    pools = group // 2
    me = lax.axis_index(GROUP_AXES)

    def iota(shape, axis):
        return lax.broadcasted_iota(jnp.int32, shape, axis)

    def onehot(cond):
        return jnp.where(cond, 1.0, 0.0).astype(BF16)

    before_tok = onehot(iota((tok, tok), 0) < iota((tok, tok), 1))
    before_pool = onehot(iota((pools, pools), 1) < iota((pools, pools), 0))
    pair = onehot(iota((pools, group), 1) // 2 == iota((pools, group), 0))
    spread = onehot(iota((group, pools), 0) // 2 == iota((group, pools), 1))
    prev = onehot((iota((group, group), 1) + 1 == iota((group, group), 0)) & (iota((group, group), 0) % 2 == 1))
    lane_p = iota((pools, tok), 1)
    pool_id = iota((pools, tok), 0)
    lane_s = iota((group, tok), 1)

    def to_int(v):
        return v.astype(jnp.int32)

    for layer in range(layers):
        off = jnp.zeros((pools, tok), jnp.int32)
        lo = jnp.zeros((group, tok), jnp.int32)
        tab_y = jnp.zeros((pools, tok), jnp.int32)
        tab_s = jnp.zeros((group, tok), jnp.int32)
        rows_x = []
        for e in range(local):
            target = me * local + e
            hit = ids_ref[:, layer * top, :] == target
            for k in range(1, top):
                hit = hit | (ids_ref[:, layer * top + k, :] == target)
            hitb = onehot(hit)
            rank = to_int(dot(hitb, before_tok))
            count = jnp.broadcast_to(jnp.sum(jnp.where(hit, 1.0, 0.0), axis=1, keepdims=True), (group, tok))
            countb = count.astype(BF16)
            count = to_int(count)
            number = to_int(dot(pair, countb))
            chunks = lax.shift_right_logical(number + (CHUNK - 1), 4)
            base = to_int(dot(before_pool, chunks.astype(F32).astype(BF16)))
            offs = to_int(dot(spread, (off * CHUNK).astype(F32).astype(BF16)))
            shift = offs + to_int(dot(prev, countb))
            key_ref[layer * local + e] = jnp.where(hit, rank + shift, -1)
            rows_x.append(jnp.sum(jnp.where((lane_p >= base) & (lane_p < base + chunks), pool_id * pool_chunks + off + lane_p - base, 0).astype(F32),
                                  axis=0, keepdims=True))
            tab_y = jnp.where((lane_p >= off) & (lane_p < off + chunks), e * cap_chunks + base + lane_p - off, tab_y)
            tab_s = jnp.where(lane_s == e, lo, tab_s)
            tab_s = jnp.where(lane_s == local + e, lo + count, tab_s)
            tab_s = jnp.where(lane_s == 2 * local + e, shift - lo, tab_s)
            off = off + chunks
            lo = lo + count
        tab_ref[layer, 0:group, :] = tab_s
        tab_ref[layer, group:group + pools, :] = tab_y
        rows_x.append(jnp.zeros((8 - local, tok), F32))
        tab_ref[layer, group + pools:group + pools + 8, :] = to_int(jnp.concatenate(rows_x, axis=0))


def tables(ids_all, layers, top, local, pool_chunks, cap_chunks):
    group, _, tok = ids_all.shape
    vm = pl.BlockSpec(memory_space=pltpu.VMEM)
    return pl.pallas_call(
        functools.partial(tables_kernel, (layers, group, top, tok, local, pool_chunks, cap_chunks)),
        out_shape=(jax.ShapeDtypeStruct((layers * local, group, tok), jnp.int32),
                   jax.ShapeDtypeStruct((layers, group + group // 2 + 8, tok), jnp.int32)),
        in_specs=[vm], out_specs=(vm, vm), name='tables',
    )(ids_all)


OFFS = (0, 1, -1, 2)
IDX = {0: 0, 1: 1, -1: 2, 2: 3}
BACK = {1: -1, -1: 1, 2: 2}


def moe_kernel(layer, dims, u_ref, a_ref, gs_ref, key_ref, tab_ref, wg_hbm, wu_hbm, wd_hbm, x_ref,
               ubuf, xg, xs, act, yq, pick, rbuf, vbuf, gmat, part, final, gsbuf, wg, wu, wd,
               ag_send, ag_recv, dd_send, dd_recv, gs_send, gs_recv, p1_send, p1_recv, p2_send, p2_recv, wsem):
    ny, nx, tok, width, local, top, pool_chunks, cap_chunks = dims
    pools = ny * nx
    group = 2 * pools
    pool_rows = pool_chunks * CHUNK
    half = tok // 2
    quarter = width // 4
    y = lax.axis_index('pool')
    ep = lax.axis_index('ep')
    x = ep // 2
    core = lax.rem(ep, 2)
    other = 1 - core

    def mod(v, n):
        return lax.rem(v + n, n)

    def at(dx, dy):
        return mod(x + dx, nx), mod(y + dy, ny)

    def dev(dx, dy, c):
        px, py = at(dx, dy)
        return {'pool': py, 'ep': px * 2 + c}

    def number(dx, dy, c):
        px, py = at(dx, dy)
        return py * (2 * nx) + px * 2 + c

    def axes(h, first, second):
        return (first, second) if h == 0 else (second, first)

    w_copies = [[pltpu.make_async_copy(src.at[layer, e], dst.at[e], wsem.at[i, e])
                 for i, (src, dst) in enumerate(((wg_hbm, wg), (wu_hbm, wu), (wd_hbm, wd)))] for e in range(local)]

    barrier = pltpu.get_barrier_semaphore()
    partners = [(0, 0, other)]
    for d in OFFS[1:]:
        for c in (0, 1):
            partners += [(d, 0, c), (0, d, c)]
    for dx, dy, c in partners:
        pl.semaphore_signal(barrier, inc=1, device_id=dev(dx, dy, c), device_id_type=MESH)
    pl.semaphore_wait(barrier, len(partners))

    def piece(h, r, q, p=None):
        if q == 0:
            step = 1 if (r == -1 or (r == 2 and p == 0)) else -1
            own = (0, 0) if r in (1, -1) else (-step, 0)
            to = (step, 0)
        else:
            step = 1 if (q == -1 or (q == 2 and p == 0)) else -1
            own = (r, 0) if q in (1, -1) else (r, -step)
            to = (0, step)
        rows = pl.ds(h * half, half) if p is None else pl.ds(h * half + p * (half // 2), half // 2)
        owner = number(*axes(h, *own), core)
        src = u_ref.at[rows] if own == (0, 0) else ubuf.at[owner, rows]
        sem = ((h * 4 + IDX[r]) * 4 + IDX[q]) * 2 + (p or 0)
        return pltpu.make_async_remote_copy(
            src_ref=src, dst_ref=ubuf.at[owner, rows], send_sem=ag_send.at[sem], recv_sem=ag_recv.at[sem],
            device_id=dev(*axes(h, *to), core), device_id_type=MESH)

    def across(h, r, q):
        rows = pl.ds(h * half, half)
        owner = number(*axes(h, r, q), core)
        src = u_ref.at[rows] if (r, q) == (0, 0) else ubuf.at[owner, rows]
        sem = (h * 4 + IDX[r]) * 4 + IDX[q]
        return pltpu.make_async_remote_copy(
            src_ref=src, dst_ref=ubuf.at[owner, rows], send_sem=dd_send.at[sem], recv_sem=dd_recv.at[sem],
            device_id=dev(0, 0, other), device_id_type=MESH)

    def gate_copy(h, q):
        back = IDX[BACK[q]]
        sem = h * 4 + back
        return pltpu.make_async_remote_copy(
            src_ref=gs_ref, dst_ref=gsbuf.at[h, back], send_sem=gs_send.at[sem], recv_sem=gs_recv.at[sem],
            device_id=dev(*axes(h, 0, q), core), device_id_type=MESH)

    started = []

    def go(copy):
        copy.start()
        started.append(copy)

    have = set()
    done = set()
    prow = lax.broadcasted_iota(jnp.int32, (pool_rows, tok), 0)

    def gather(dx, dy):
        px, py = at(dx, dy)
        chip = py * nx + px
        across(0, dx, dy).wait_recv()
        across(1, dy, dx).wait_recv()
        halves = []
        for par in range(2):
            hit = None
            for e in range(local):
                this = prow == key_ref[layer * local + e, pl.ds(2 * chip + par, 1), :]
                hit = this if hit is None else hit | this
            halves.append(jnp.where(hit, 1.0, 0.0).astype(BF16))
        onehot = jnp.concatenate(halves, axis=1)
        rows = ubuf[pl.ds(2 * chip, 2)].reshape(2 * tok, width)
        xg[pl.ds(chip * pool_chunks, pool_chunks)] = dot(onehot, rows).astype(BF16).reshape(pool_chunks, CHUNK, width)

    def ready(limit):
        for dy in OFFS:
            for dx in OFFS:
                if limit and (dx, dy) not in done and (0, dx, dy) in have and (1, dy, dx) in have:
                    done.add((dx, dy))
                    gather(dx, dy)
                    limit -= 1

    for h in (0, 1):
        go(piece(h, -1, 0))
        go(piece(h, 1, 0))
    for h in (0, 1):
        go(across(h, 0, 0))
        go(piece(h, 0, -1))
        go(piece(h, 0, 1))
    for h in (0, 1):
        for q in OFFS[1:]:
            go(gate_copy(h, q))
        have.add((h, 0, 0))
    for e in range(local):
        for cp in w_copies[e]:
            cp.start()
    ubuf[number(0, 0, core)] = u_ref[...]

    for r, p in ((-1, 0), (1, 1)):
        for h in (0, 1):
            piece(h, r, 0).wait_recv()
            go(piece(h, 2, 0, p))
            go(piece(h, r, -1))
            go(piece(h, r, 1))
            go(across(h, r, 0))
            have.add((h, r, 0))
        ready(1)
    for h in (0, 1):
        piece(h, 2, 0, 0).wait_recv()
        piece(h, 2, 0, 1).wait_recv()
        go(piece(h, 2, -1))
        go(piece(h, 2, 1))
        go(across(h, 2, 0))
        have.add((h, 2, 0))
    for r in OFFS:
        for q, p in ((-1, 0), (1, 1)):
            for h in (0, 1):
                piece(h, r, q).wait_recv()
                go(piece(h, r, 2, p))
                go(across(h, r, q))
                have.add((h, r, q))
            ready(1)
    for r in OFFS:
        for h in (0, 1):
            piece(h, r, 2, 0).wait_recv()
            piece(h, r, 2, 1).wait_recv()
            go(across(h, r, 2))
            have.add((h, r, 2))
        ready(2)
    ready(pools)

    tab_y0 = group
    tab_x0 = group + pools
    for e in range(local):
        def move(i, carry, e=e):
            xs[e * cap_chunks + i] = xg[tab_ref[layer, tab_x0 + e, i]]
            return carry
        lax.fori_loop(0, cap_chunks, move, 0, unroll=8)
    per = TILE // CHUNK
    for e in range(local):
        for cp in w_copies[e]:
            cp.wait()

        def tile(i, carry, e=e):
            rows = pl.ds(e * cap_chunks + i * per, per)
            rows_in = xs[rows].reshape(TILE, width)
            first = dot(rows_in, wg[e])
            second = dot(rows_in, wu[e])
            act[pl.ds(e * (cap_chunks // per) + i, 1)] = (first * (1.0 / (1.0 + jnp.exp(-first))) * second).astype(BF16)[None]
            return carry

        lax.fori_loop(0, cap_chunks // per, tile, 0)

    jrow = lax.broadcasted_iota(jnp.int32, (WINDOW, pool_rows), 0)
    diff = lax.broadcasted_iota(jnp.int32, (WINDOW, pool_rows), 1) - jrow

    def choose(chip, carry):
        halves = []
        for par in range(2):
            hit = None
            for e in range(local):
                lo = tab_ref[layer, 2 * chip + par, e]
                hi = tab_ref[layer, 2 * chip + par, local + e]
                delta = tab_ref[layer, 2 * chip + par, 2 * local + e]
                this = (diff == delta) & (jrow >= lo) & (jrow < hi)
                hit = this if hit is None else hit | this
            halves.append(jnp.where(hit, 1.0, 0.0).astype(BF16))
        pick[chip] = jnp.concatenate(halves, axis=0)
        return carry

    lax.fori_loop(0, pools, choose, 0)

    def first_copy(h, w, r, flip):
        c = other if flip else core
        mine = (x, y)[h]
        there = at(r, r)[h]
        sem = ((h * 2 + w) * 4 + IDX[r]) * 2 + flip
        return pltpu.make_async_remote_copy(
            src_ref=rbuf.at[h * 2 + w, there, c], dst_ref=vbuf.at[h * 2 + w, mine, core],
            send_sem=p1_send.at[sem], recv_sem=p1_recv.at[sem], device_id=dev(*axes(h, r, 0), c), device_id_type=MESH)

    def second_copy(h, w, q):
        sem = (h * 2 + w) * 4 + IDX[q]
        return pltpu.make_async_remote_copy(
            src_ref=part.at[h * 2 + w, IDX[q]], dst_ref=final.at[h * 2 + w, IDX[q]],
            send_sem=p2_send.at[sem], recv_sem=p2_recv.at[sem], device_id=dev(*axes(h, 0, q), core), device_id_type=MESH)

    firsts = [(2, 0), (2, 1), (1, 0), (-1, 0), (1, 1), (-1, 1), (0, 1)]
    order = [(0, 0), (1, 0), (0, 1), (1, 1)]
    for h, w in order:
        n = h * 2 + w
        cols = slice(n * quarter, (n + 1) * quarter)
        for e in range(local):
            def down(i, carry, e=e):
                out = dot(act[e * (cap_chunks // per) + i], wd[e, :, cols])
                yq[pl.ds(e * cap_chunks + i * per, per)] = out.astype(BF16).reshape(per, CHUNK, quarter)
                return carry
            lax.fori_loop(0, cap_chunks // per, down, 0)

        def window(chip, carry):
            rows = jnp.concatenate([yq[tab_ref[layer, tab_y0 + chip, i]] for i in range(pool_chunks)], axis=0)
            out = dot(pick[chip], rows).astype(BF16)
            cy = chip // nx
            cx = chip % nx
            one, two = (cx, cy) if h == 0 else (cy, cx)
            for par in range(2):
                rbuf[n, one, par, two] = out[par * WINDOW:(par + 1) * WINDOW]
            return carry

        lax.fori_loop(0, pools, window, 0)
        mine = (x, y)[h]
        vbuf[n, mine, core] = rbuf[n, mine, core]
        for r, flip in firsts:
            go(first_copy(h, w, r, flip))

    slots = vbuf.shape[1] * vbuf.shape[2] * WINDOW
    srow = lax.broadcasted_iota(jnp.int32, (slots, tok), 0)
    for h in (0, 1):
        for q in OFFS:
            if q:
                gate_copy(h, BACK[q]).wait_recv()
                gs = gsbuf[h, IDX[q]]
            else:
                gs = gs_ref[...]
            slot = gs[top:2 * top].astype(jnp.int32)
            if h == 0:
                rel = slot - y * slots
            else:
                source = lax.shift_right_logical(slot, 6)
                sx = lax.shift_right_logical(source, 1) & (nx - 1)
                sy = source // (2 * nx)
                rel = jnp.where(sx == x, (sy * 2 + (source & 1)) * WINDOW + (slot & (WINDOW - 1)), -1)
            g = jnp.zeros((slots, tok), F32)
            for k in range(top):
                g = jnp.where(srow == rel[k:k + 1], gs[k:k + 1], g)
            for i, v in enumerate(split3(jnp.transpose(g))):
                gmat[h * 4 + IDX[q], i * tok:(i + 1) * tok, :] = v

    for h, w in order:
        n = h * 2 + w
        for r, flip in firsts:
            first_copy(h, w, r, flip).wait_recv()
        for q in (2, 1, -1, 0):
            two = at(q, q)[1 - h]
            parts = dot(gmat[h * 4 + IDX[q]], vbuf[n, :, :, two].reshape(slots, quarter))
            part[n, IDX[q]] = parts[0:tok] + parts[tok:2 * tok] + parts[2 * tok:3 * tok]
            if q:
                go(second_copy(h, w, q))
    for h, w in order:
        n = h * 2 + w
        cols = slice(n * quarter, (n + 1) * quarter)
        for q in OFFS[1:]:
            second_copy(h, w, q).wait_recv()
        total = (part[n, 0] + final[n, 1]) + (final[n, 2] + final[n, 3])
        x_ref[:, cols] = (a_ref[:, cols].astype(F32) + total).astype(BF16)
    for copy in started:
        copy.wait_send()


def moe(layer, mesh_dims, a, u, gs, keys, tab, w_gate, w_up, w_down, pool_chunks, cap_chunks):
    ny, nx = mesh_dims
    tok, width = u.shape
    top = gs.shape[0] // 2
    local, ff = w_gate.shape[1], w_gate.shape[3]
    pools = ny * nx
    group = 2 * pools
    quarter = width // 4
    per = TILE // CHUNK
    vm = pl.BlockSpec(memory_space=pltpu.VMEM)
    hb = pl.BlockSpec(memory_space=pl.ANY)
    sm = pl.BlockSpec(memory_space=pltpu.SMEM)
    sem = pltpu.SemaphoreType.DMA
    return pl.pallas_call(
        functools.partial(moe_kernel, layer, (ny, nx, tok, width, local, top, pool_chunks, cap_chunks)),
        out_shape=jax.ShapeDtypeStruct((tok, width), BF16),
        in_specs=[vm, vm, vm, vm, sm, hb, hb, hb],
        out_specs=vm,
        scratch_shapes=[
            pltpu.VMEM((group, tok, width), BF16),
            pltpu.VMEM((pools * pool_chunks, CHUNK, width), BF16),
            pltpu.VMEM((local * cap_chunks, CHUNK, width), BF16),
            pltpu.VMEM((local * cap_chunks // per, TILE, ff), BF16),
            pltpu.VMEM((local * cap_chunks, CHUNK, quarter), BF16),
            pltpu.VMEM((pools, 2 * WINDOW, pool_chunks * CHUNK), BF16),
            pltpu.VMEM((4, nx, 2, ny, WINDOW, quarter), BF16),
            pltpu.VMEM((4, nx, 2, ny, WINDOW, quarter), BF16),
            pltpu.VMEM((8, 3 * tok, 2 * nx * WINDOW), BF16),
            pltpu.VMEM((4, 4, tok, quarter), F32),
            pltpu.VMEM((4, 4, tok, quarter), F32),
            pltpu.VMEM((2, 4) + gs.shape, F32),
            pltpu.VMEM((local, width, ff), BF16), pltpu.VMEM((local, width, ff), BF16), pltpu.VMEM((local, ff, width), BF16),
            sem((64,)), sem((64,)), sem((32,)), sem((32,)), sem((8,)), sem((8,)), sem((32,)), sem((32,)), sem((16,)), sem((16,)), sem((3, local)),
        ],
        compiler_params=pltpu.CompilerParams(vmem_limit_bytes=VMEM_LIMIT, collective_id=layer, has_side_effects=True),
        cost_estimate=pl.CostEstimate(flops=6 * 10 ** 9, bytes_accessed=20 * 10 ** 6, transcendentals=0),
        name='moe',
    )(u, a, gs, keys, tab, w_gate, w_up, w_down)


def solution(mesh):
    ny, nx = mesh.shape['pool'], mesh.shape['ep'] // 2

    def device_step(hidden, k_cache, v_cache, lengths, w_query, w_key, w_value, w_out, w_router, expert_ids, w_gate, w_up, w_down):
        tok, width = hidden.shape
        layers, _, top = expert_ids.shape
        local = w_gate.shape[1]
        group = 2 * nx * ny
        pools = nx * ny
        k_cache = k_cache.reshape(layers, tok, k_cache.shape[2], k_cache.shape[4])
        v_cache = v_cache.reshape(k_cache.shape)
        mine = jnp.swapaxes(expert_ids, 1, 2).reshape(layers * top, tok)
        pool_chunks = (2 * (WINDOW - 1) + local * (CHUNK - 1)) // CHUNK
        most = 2 * group * tok * top // (group * local)
        cap_chunks = pl.cdiv((most + pools * (CHUNK - 1)) // CHUNK, TILE // CHUNK) * (TILE // CHUNK)
        for layer in range(layers):
            out = attention(layer, None if layer else (ny, 2 * nx), hidden, k_cache, v_cache, lengths, w_query, w_key, w_value, w_out, w_router,
                            expert_ids[layer], mine, local)
            if layer == 0:
                keys, tab = tables(out[3], layers, top, local, pool_chunks, cap_chunks)
            a, u, gs = out[:3]
            hidden = moe(layer, (ny, nx), a, u, gs, keys, tab, w_gate, w_up, w_down, pool_chunks, cap_chunks)
        return hidden

    cache_spec = P(None, BATCH_AXES, None, None, None)
    expert_spec = P(None, GROUP_AXES, None, None)
    in_specs = (P(BATCH_AXES, None), cache_spec, cache_spec, P(BATCH_AXES), P(), P(), P(), P(), P(), P(None, BATCH_AXES, None), expert_spec, expert_spec, expert_spec)
    return jax.shard_map(device_step, mesh=mesh, in_specs=in_specs, out_specs=P(BATCH_AXES, None), check_vma=False)
```

```python
import functools

import jax
import jax.numpy as jnp
from jax import lax
from jax.experimental import pallas as pl
from jax.experimental.pallas import tpu as pltpu
from jax.sharding import PartitionSpec as P

EPS = 1e-6
GROUP_AXES = ('pool', 'ep')
BATCH_AXES = ('dp', 'pool', 'ep')
F32 = jnp.float32
BF16 = jnp.bfloat16
I32 = jnp.int32
CHUNK = 16
WINDOW = 64
TILE = 256
LANES = 128
BLOCK = 16
WAVES = 2
MESH = pl.DeviceIdType.MESH
OFFS = (0, -1, 1, 2)
IDX = {0: 0, 1: 1, -1: 2, 2: 3}
BACK = {1: -1, -1: 1, 2: 2}


def rms_norm(wide):
    return (wide * lax.rsqrt(jnp.mean(wide * wide, axis=-1, keepdims=True) + EPS)).astype(BF16)


def dot(a, b):
    return jnp.dot(a, b, preferred_element_type=F32)


def dot_t(a, b):
    return lax.dot_general(a, b, (((1,), (1,)), ((), ())), preferred_element_type=F32)


def split3(w):
    hi = w.astype(BF16)
    rest = w - hi.astype(F32)
    mid = rest.astype(BF16)
    low = (rest - mid.astype(F32)).astype(BF16)
    return hi, mid, low


def iota(shape, axis):
    return lax.broadcasted_iota(I32, shape, axis)


def onehot(cond):
    return jnp.where(cond, 1.0, 0.0).astype(BF16)


def step_kernel(dims, hidden_ref, kc_hbm, vc_hbm, len_ref, wq_hbm, wk_hbm, wv_hbm, wo_hbm, wr_hbm, cols_ref, mine_ref, wg_hbm, wu_hbm, wd_hbm,
                x_ref,
                xcur, abuf, ubuf0, gs, q3, o3, sbuf, nbuf, kn3, vn3, wq, wk, wv, wo, wr,
                idsbuf, keys, tabv, tab, ubuf, xg, xt, act, yq, pick, rbuf, vbuf, gmat, part, final, gsbuf, wg, wu, wd,
                ksem, vsem, asem, wsem, tsem, id_send, id_recv, ag_send, ag_recv, dd_send, dd_recv, gs_send, gs_recv,
                p1_send, p1_recv, p2_send, p2_recv):
    ny, nx, layers, tok, width, heads, hd, seq, experts, local, top, pool_chunks, cap_chunks = dims
    pools = ny * nx
    group = 2 * pools
    pool_rows = pool_chunks * CHUNK
    span = tok // WAVES
    half = span // 2
    quarter = width // 4
    lane_tiles = quarter // LANES
    per = TILE // CHUNK
    per_expert = cap_chunks // per
    slots = 2 * nx * WINDOW
    y = lax.axis_index('pool')
    ep = lax.axis_index('ep')
    x = ep // 2
    core = lax.rem(ep, 2)
    other = 1 - core
    me = y * (2 * nx) + ep

    def at(dx, dy):
        return lax.rem(x + dx + nx, nx), lax.rem(y + dy + ny, ny)

    def dev(dx, dy, c):
        px, py = at(dx, dy)
        return {'pool': py, 'ep': px * 2 + c}

    def number(dx, dy, c):
        px, py = at(dx, dy)
        return py * (2 * nx) + px * 2 + c

    def axes(h, first, second):
        return (first, second) if h == 0 else (second, first)

    def peer(d):
        to = lax.rem(me + d, group)
        return {'pool': to // (2 * nx), 'ep': lax.rem(to, 2 * nx)}

    def remote(src, dst, send, recv, device):
        return pltpu.make_async_remote_copy(src_ref=src, dst_ref=dst, send_sem=send, recv_sem=recv, device_id=device, device_id_type=MESH)

    def att_copies(layer):
        return [pltpu.make_async_copy(src.at[layer], dst, asem.at[i])
                for i, (src, dst) in enumerate(((wq_hbm, wq), (wk_hbm, wk), (wv_hbm, wv), (wo_hbm, wo), (wr_hbm, wr)))]

    def expert_copies(layer):
        return [pltpu.make_async_copy(src.at[layer, e], dst.at[e], wsem.at[i, e])
                for i, (src, dst) in enumerate(((wg_hbm, wg), (wu_hbm, wu), (wd_hbm, wd))) for e in range(local)]

    def kv_copies(layer, b):
        rows = pl.ds(b * (BLOCK * seq), BLOCK * seq)
        return (pltpu.make_async_copy(kc_hbm.at[layer, rows], rbuf.at[rows], ksem.at[b]),
                pltpu.make_async_copy(vc_hbm.at[layer, rows], vbuf.at[rows], vsem.at[b]))

    def id_copy(d):
        return remote(mine_ref, idsbuf.at[me], id_send.at[d], id_recv.at[d], peer(d))

    def piece(w, h, r, q, p=None):
        if q == 0:
            step = 1 if (r == -1 or (r == 2 and p == 0)) else -1
            own = (0, 0) if r in (1, -1) else (-step, 0)
            to = (step, 0)
        else:
            step = 1 if (q == -1 or (q == 2 and p == 0)) else -1
            own = (r, 0) if q in (1, -1) else (r, -step)
            to = (0, step)
        first = w * span + h * half
        rows = pl.ds(first, half) if p is None else pl.ds(first + p * (half // 2), half // 2)
        owner = number(*axes(h, *own), core)
        src = ubuf0.at[rows] if own == (0, 0) else ubuf.at[owner, rows]
        sem = (((w * 2 + h) * 4 + IDX[r]) * 4 + IDX[q]) * 2 + (p or 0)
        return remote(src, ubuf.at[owner, rows], ag_send.at[sem], ag_recv.at[sem], dev(*axes(h, *to), core))

    def across(w, h, r, q):
        rows = pl.ds(w * span + h * half, half)
        owner = number(*axes(h, r, q), core)
        src = ubuf0.at[rows] if (r, q) == (0, 0) else ubuf.at[owner, rows]
        sem = ((w * 2 + h) * 4 + IDX[r]) * 4 + IDX[q]
        return remote(src, ubuf.at[owner, rows], dd_send.at[sem], dd_recv.at[sem], dev(0, 0, other))

    def gate_copy(h, q):
        back = IDX[BACK[q]]
        sem = h * 4 + back
        return remote(gs, gsbuf.at[h, back], gs_send.at[sem], gs_recv.at[sem], dev(*axes(h, 0, q), core))

    def window_row(n, one, c, two=0):
        return ((n * nx + one) * 2 + c) * (ny * lane_tiles * WINDOW) + two * (lane_tiles * WINDOW)

    def first_copy(h, w, r, flip):
        n = h * 2 + w
        c = other if flip else core
        size = ny * lane_tiles * WINDOW
        src = pl.ds(pl.multiple_of(window_row(n, at(r, r)[h], c), size), size)
        dst = pl.ds(pl.multiple_of(window_row(n, (x, y)[h], core), size), size)
        sem = (n * 4 + IDX[r]) * 2 + flip
        return remote(rbuf.at[src], vbuf.at[dst], p1_send.at[sem], p1_recv.at[sem], dev(*axes(h, r, 0), c))

    def second_copy(h, w, q):
        n = h * 2 + w
        sem = n * 4 + IDX[q]
        return remote(part.at[n, IDX[q]], final.at[n, IDX[q]], p2_send.at[sem], p2_recv.at[sem], dev(*axes(h, 0, q), core))

    for cp in att_copies(0):
        cp.start()
    barrier = pltpu.get_barrier_semaphore()
    for d in range(1, group):
        pl.semaphore_signal(barrier, inc=1, device_id=peer(d), device_id_type=MESH)
    pl.semaphore_wait(barrier, group - 1)
    for d in range(1, group):
        id_copy(d).start()
    idsbuf[me] = mine_ref[...]
    xcur[...] = hidden_ref[...]
    scale = hd ** -0.5
    lane = iota((heads, seq), 1)

    def layer_body(layer, carry):
        for b in range(tok // BLOCK):
            for cp in kv_copies(layer, b):
                cp.start()
        for cp in expert_copies(layer):
            cp.start()
        normed = rms_norm(xcur[...].astype(F32))
        for cp in att_copies(layer)[:3]:
            cp.wait()
        kn3[...] = dot(normed, wk[...]).astype(BF16).astype(F32)
        vn3[...] = dot(normed, wv[...]).astype(BF16).astype(F32)
        for h in range(heads):
            if h % 2 == 0:
                pair = dot(normed, wq[:, h * hd:(h + 2) * hd])
            q3[:, h, :] = pair[:, (h % 2) * hd:(h % 2 + 1) * hd].astype(BF16).astype(F32)

        def block(b, c2):
            kcp, vcp = kv_copies(layer, b)
            kcp.wait()
            for j in range(BLOCK):
                t = b * BLOCK + j
                q = q3[t]
                s = dot_t(q.astype(BF16), rbuf[pl.ds(t * seq, seq), :]) * scale
                sbuf[j * heads:(j + 1) * heads, :] = jnp.where(lane < len_ref[t], s, -jnp.inf)
                nbuf[j * heads:(j + 1) * heads, :] = q * kn3[pl.ds(t, 1), :]
            s = sbuf[...]
            sn = jnp.sum(nbuf[...], axis=1, keepdims=True) * scale
            peak = jnp.maximum(jnp.max(s, axis=1, keepdims=True), sn)
            p = jnp.exp(s - peak)
            pn = jnp.exp(sn - peak)
            inv = 1.0 / (jnp.sum(p, axis=1, keepdims=True) + pn)
            pb = (p * inv).astype(BF16)
            pnb = (pn * inv).astype(BF16).astype(F32)
            vcp.wait()
            for j in range(BLOCK):
                t = b * BLOCK + j
                rows = slice(j * heads, (j + 1) * heads)
                o = dot(pb[rows], vbuf[pl.ds(t * seq, seq), :]) + pnb[rows] * vn3[pl.ds(t, 1), :]
                o3[t] = o.astype(BF16).astype(F32)
            return c2

        def project(w):
            rows = slice(w * span, (w + 1) * span)
            mixed = jnp.concatenate([o3[rows, h, :].astype(BF16) for h in range(heads)], axis=1)
            a = (xcur[rows].astype(F32) + dot(mixed, wo[...])).astype(BF16)
            abuf[rows] = a
            ubuf0[rows] = rms_norm(a.astype(F32))

        started = []

        def go(fn, *args):
            fn(*args).start()
            started.append((fn, args))

        have = set()
        done = set()
        prow = iota((pool_rows, tok), 0)

        def gather(dx, dy):
            px, py = at(dx, dy)
            chip = py * nx + px
            for w in range(WAVES):
                across(w, 0, dx, dy).wait_recv()
                across(w, 1, dy, dx).wait_recv()
            halves = []
            for par in range(2):
                hit = None
                for e in range(local):
                    this = prow == keys[e, pl.ds(2 * chip + par, 1), :]
                    hit = this if hit is None else hit | this
                halves.append(onehot(hit))
            rows = ubuf[pl.ds(2 * chip, 2)].reshape(2 * tok, width)
            xg[pl.ds(chip * pool_chunks, pool_chunks)] = dot(jnp.concatenate(halves, axis=1), rows).astype(BF16).reshape(pool_chunks, CHUNK, width)

        def ready(limit):
            for dy in OFFS:
                for dx in OFFS:
                    if limit and (dx, dy) not in done and all((w, 0, dx, dy) in have and (w, 1, dy, dx) in have for w in range(WAVES)):
                        done.add((dx, dy))
                        gather(dx, dy)
                        limit -= 1

        def s0(w):
            for h in (0, 1):
                go(piece, w, h, -1, 0)
                go(piece, w, h, 1, 0)
            for h in (0, 1):
                go(piece, w, h, 0, -1)
                go(piece, w, h, 0, 1)
                go(across, w, h, 0, 0)
                have.add((w, h, 0, 0))

        def s2(w):
            for r, p in ((-1, 0), (1, 1)):
                for h in (0, 1):
                    piece(w, h, r, 0).wait_recv()
                    go(piece, w, h, 2, 0, p)
                    go(piece, w, h, r, -1)
                    go(piece, w, h, r, 1)
                    go(across, w, h, r, 0)
                    have.add((w, h, r, 0))

        def s3(w):
            for h in (0, 1):
                piece(w, h, 2, 0, 0).wait_recv()
                piece(w, h, 2, 0, 1).wait_recv()
                go(piece, w, h, 2, -1)
                go(piece, w, h, 2, 1)
                go(across, w, h, 2, 0)
                have.add((w, h, 2, 0))

        def s4(w, r):
            for q, p in ((-1, 0), (1, 1)):
                for h in (0, 1):
                    piece(w, h, r, q).wait_recv()
                    go(piece, w, h, r, 2, p)
                    go(across, w, h, r, q)
                    have.add((w, h, r, q))

        def s5(w, r):
            for h in (0, 1):
                piece(w, h, r, 2, 0).wait_recv()
                piece(w, h, r, 2, 1).wait_recv()
                go(across, w, h, r, 2)
                have.add((w, h, r, 2))

        blocks = span // BLOCK
        lax.fori_loop(0, blocks, block, 0)
        att_copies(layer)[3].wait()
        project(0)
        s0(0)
        lax.fori_loop(blocks, 2 * blocks - 1, block, 0)
        s2(0)
        lax.fori_loop(2 * blocks - 1, 2 * blocks, block, 0)
        s4(0, 0)
        project(1)
        s0(1)
        s3(0)

        att_copies(layer)[4].wait()
        hi, mid, low = split3(wr[...])
        u = ubuf0[...]
        logits = dot(u, hi) + dot(u, mid) + dot(u, low)

        @pl.when(layer + 1 < layers)
        def _():
            for cp in att_copies(layer + 1):
                cp.start()

        e_iota = iota((tok, experts), 1)
        before = onehot(iota((tok, tok), 1) < iota((tok, tok), 0))
        e_row = iota((experts, experts), 0)
        e_col = iota((experts, experts), 1)
        same = onehot((e_row < e_col) & (e_row // local == e_col // local))
        hits = [cols_ref[layer, :, k:k + 1] == e_iota for k in range(top)]
        chosen = hits[0]
        for k in range(1, top):
            chosen = chosen | hits[k]
        chosen = jnp.where(chosen, 1.0, 0.0)
        rank = dot(before, chosen.astype(BF16))
        count = jnp.sum(chosen, axis=0, keepdims=True)
        start = dot(jnp.broadcast_to(count, (8, experts)).astype(BF16), same)[0:1]
        slot_full = rank + start + ((e_iota // local) * WINDOW).astype(F32)
        picked = [jnp.sum(jnp.where(hit, logits, 0.0), axis=1, keepdims=True) for hit in hits]
        peak = picked[0]
        for k in range(1, top):
            peak = jnp.maximum(peak, picked[k])
        ex = [jnp.exp(v - peak) for v in picked]
        total = ex[0]
        for k in range(1, top):
            total = total + ex[k]
        columns = [v / total for v in ex] + [jnp.sum(jnp.where(hit, slot_full, 0.0), axis=1, keepdims=True) for hit in hits]
        columns.append(jnp.zeros((tok, LANES - 2 * top), F32))
        gs[...] = jnp.transpose(jnp.concatenate(columns, axis=1))[:2 * top]
        ubuf[me] = u
        for h in (0, 1):
            for q in OFFS[1:]:
                go(gate_copy, h, q)
        s4(0, -1)
        s4(0, 1)
        s2(1)

        @pl.when(layer == 0)
        def _():
            for d in range(1, group):
                id_copy(d).wait()

        before_tok = onehot(iota((tok, tok), 0) < iota((tok, tok), 1))
        before_pool = onehot(iota((pools, pools), 1) < iota((pools, pools), 0))
        pair_of = onehot(iota((pools, group), 1) // 2 == iota((pools, group), 0))
        spread = onehot(iota((group, pools), 0) // 2 == iota((group, pools), 1))
        prev = onehot((iota((group, group), 1) + 1 == iota((group, group), 0)) & (iota((group, group), 0) % 2 == 1))
        lane_p = iota((pools, tok), 1)
        pool_id = iota((pools, tok), 0)
        lane_s = iota((group, tok), 1)
        off = jnp.zeros((pools, tok), I32)
        lo = jnp.zeros((group, tok), I32)
        tab_y = jnp.zeros((pools, tok), I32)
        tab_s = jnp.zeros((group, tok), I32)
        rows_x = []
        for e in range(local):
            target = me * local + e
            hit = idsbuf[:, layer, 0, :] == target
            for k in range(1, top):
                hit = hit | (idsbuf[:, layer, k, :] == target)
            hitb = onehot(hit)
            rank = dot(hitb, before_tok).astype(I32)
            count = jnp.broadcast_to(jnp.sum(jnp.where(hit, 1.0, 0.0), axis=1, keepdims=True), (group, tok))
            countb = count.astype(BF16)
            count = count.astype(I32)
            amount = dot(pair_of, countb).astype(I32)
            chunks = lax.shift_right_logical(amount + (CHUNK - 1), 4)
            base = dot(before_pool, chunks.astype(F32).astype(BF16)).astype(I32)
            shift = dot(spread, (off * CHUNK).astype(F32).astype(BF16)).astype(I32) + dot(prev, countb).astype(I32)
            keys[e] = jnp.where(hit, rank + shift, -1)
            rows_x.append(jnp.sum(jnp.where((lane_p >= base) & (lane_p < base + chunks), pool_id * pool_chunks + off + lane_p - base, 0).astype(F32),
                                  axis=0, keepdims=True))
            tab_y = jnp.where((lane_p >= off) & (lane_p < off + chunks), e * cap_chunks + base + lane_p - off, tab_y)
            tab_s = jnp.where(lane_s == e, lo, tab_s)
            tab_s = jnp.where(lane_s == local + e, lo + count, tab_s)
            tab_s = jnp.where(lane_s == 2 * local + e, shift - lo, tab_s)
            off = off + chunks
            lo = lo + count
        tab_y0 = group
        tab_x0 = group + pools
        tabv[0:group, :] = tab_s
        tabv[group:group + pools, :] = jnp.clip(tab_y, 0, local * cap_chunks - 1)
        rows_x.append(jnp.zeros((8 - local, tok), F32))
        tabv[tab_x0:tab_x0 + 8, :] = jnp.clip(jnp.concatenate(rows_x, axis=0).astype(I32), 0, pools * pool_chunks - 1)
        tab_copy = pltpu.make_async_copy(tabv, tab, tsem)
        tab_copy.start()

        s4(0, 2)
        s3(1)
        for r in OFFS:
            s5(0, r)
        ready(1)
        s4(1, 0)
        ready(2)

        srow = iota((slots, tok), 0)

        def gates(h):
            for q in OFFS:
                if q:
                    gate_copy(h, BACK[q]).wait_recv()
                    table = gsbuf[h, IDX[q]]
                else:
                    table = gs[...]
                slot = table[top:2 * top].astype(I32)
                if h == 0:
                    rel = slot - y * slots
                else:
                    source = lax.shift_right_logical(slot, 6)
                    sx = lax.shift_right_logical(source, 1) & (nx - 1)
                    sy = source // (2 * nx)
                    rel = jnp.where(sx == x, (sy * 2 + (source & 1)) * WINDOW + (slot & (WINDOW - 1)), -1)
                g = jnp.zeros((slots, tok), F32)
                for k in range(top):
                    g = jnp.where(srow == rel[k:k + 1], table[k:k + 1], g)
                for i, v in enumerate(split3(jnp.transpose(g))):
                    gmat[h * 4 + IDX[q], i * tok:(i + 1) * tok, :] = v

        s4(1, -1)
        gates(0)
        s4(1, 1)
        ready(2)
        tab_copy.wait()

        jrow = iota((WINDOW, pool_rows), 0)
        diff = iota((WINDOW, pool_rows), 1) - jrow

        def choose(chip, c2):
            halves = []
            for par in range(2):
                hit = None
                for e in range(local):
                    low_ = tab[2 * chip + par, e]
                    high_ = tab[2 * chip + par, local + e]
                    delta = tab[2 * chip + par, 2 * local + e]
                    this = (diff == delta) & (jrow >= low_) & (jrow < high_)
                    hit = this if hit is None else hit | this
                halves.append(onehot(hit))
            pick[chip] = jnp.concatenate(halves, axis=0)
            return c2

        lax.fori_loop(0, pools, choose, 0)
        s4(1, 2)
        ready(3)
        gates(1)
        s5(1, 0)
        ready(2)
        s5(1, -1)
        s5(1, 1)
        ready(4)
        s5(1, 2)
        ready(pools)

        for cp in expert_copies(layer):
            cp.wait()

        def tile(i, c2):
            e = i // per_expert
            first_chunk = (i % per_expert) * per
            for j in range(per):
                xt[j * CHUNK:(j + 1) * CHUNK, :] = xg[tab[tab_x0 + e, first_chunk + j]]
            rows_in = xt[...]
            first = dot(rows_in, wg[e])
            second = dot(rows_in, wu[e])
            act[i] = (first * (1.0 / (1.0 + jnp.exp(-first))) * second).astype(BF16)
            return c2

        lax.fori_loop(0, local * per_expert, tile, 0)
        for fn, args in started:
            fn(*args).wait_send()
        started.clear()

        firsts = [(2, 0), (2, 1), (1, 0), (-1, 0), (1, 1), (-1, 1), (0, 1)]
        for w in (0, 1):
            def down(i, c2):
                out = dot(act[i], wd[i // per_expert, :, 2 * w * quarter:2 * (w + 1) * quarter])
                yq[pl.ds(i * per, per)] = out.astype(BF16).reshape(per, CHUNK, 2 * quarter)
                return c2

            lax.fori_loop(0, local * per_expert, down, 0)

            def window(chip, c2):
                rows = jnp.concatenate([yq[tab[tab_y0 + chip, i]] for i in range(pool_chunks)], axis=0)
                out = dot(pick[chip], rows).astype(BF16)
                cy = chip // nx
                cx = chip % nx
                for h in (0, 1):
                    one, two = axes(h, cx, cy)
                    for par in range(2):
                        for lt in range(lane_tiles):
                            row = window_row(h * 2 + w, one, par, two) + lt * WINDOW
                            rbuf[pl.ds(pl.multiple_of(row, WINDOW), WINDOW), :] = out[par * WINDOW:(par + 1) * WINDOW,
                                                                                     h * quarter + lt * LANES:h * quarter + (lt + 1) * LANES]
                return c2

            lax.fori_loop(0, pools, window, 0)
            for r, flip in firsts:
                for h in (0, 1):
                    go(first_copy, h, w, r, flip)
            for h in (0, 1):
                size = ny * lane_tiles * WINDOW
                own = pl.ds(pl.multiple_of(window_row(h * 2 + w, (x, y)[h], core), size), size)
                vbuf[own, :] = rbuf[own, :]

        for w in (0, 1):
            for h in (0, 1):
                n = h * 2 + w
                for r, flip in firsts:
                    first_copy(h, w, r, flip).wait_recv()
                for q in (2, 1, -1, 0):
                    two = at(q, q)[1 - h]
                    rows = []
                    for s in range(2 * nx):
                        row = window_row(n, s // 2, s % 2, two)
                        rows.append(jnp.concatenate([vbuf[pl.ds(pl.multiple_of(row + lt * WINDOW, WINDOW), WINDOW), :] for lt in range(lane_tiles)], axis=1))
                    parts = dot(gmat[h * 4 + IDX[q]], jnp.concatenate(rows, axis=0))
                    part[n, IDX[q]] = parts[0:tok] + parts[tok:2 * tok] + parts[2 * tok:3 * tok]
                    if q:
                        go(second_copy, h, w, q)
        for w in (0, 1):
            for h in (0, 1):
                n = h * 2 + w
                where = slice((w * 2 + h) * quarter, (w * 2 + h + 1) * quarter)
                for q in OFFS[1:]:
                    second_copy(h, w, q).wait_recv()
                total = (part[n, 0] + final[n, 1]) + (final[n, 2] + final[n, 3])
                xcur[:, where] = (abuf[:, where].astype(F32) + total).astype(BF16)
        for fn, args in started:
            fn(*args).wait_send()
        return carry

    lax.fori_loop(0, layers, layer_body, 0)
    x_ref[...] = xcur[...]


def solution(mesh):
    ny, nx = mesh.shape['pool'], mesh.shape['ep'] // 2

    def device_step(hidden, k_cache, v_cache, lengths, w_query, w_key, w_value, w_out, w_router, expert_ids, w_gate, w_up, w_down):
        tok, width = hidden.shape
        layers, _, top = expert_ids.shape
        seq, hd = k_cache.shape[2], k_cache.shape[4]
        heads = w_query.shape[2] // hd
        experts = w_router.shape[2]
        local, ff = w_gate.shape[1], w_gate.shape[3]
        pools = nx * ny
        group = 2 * pools
        k_cache = k_cache.reshape(layers, tok * seq, hd)
        v_cache = v_cache.reshape(layers, tok * seq, hd)
        mine = jnp.swapaxes(expert_ids, 1, 2)
        pool_chunks = (2 * (WINDOW - 1) + local * (CHUNK - 1)) // CHUNK
        most = 2 * group * tok * top // (group * local)
        per = TILE // CHUNK
        cap_chunks = pl.cdiv((most + pools * (CHUNK - 1)) // CHUNK, per) * per
        quarter = width // 4
        vm = pl.BlockSpec(memory_space=pltpu.VMEM)
        hb = pl.BlockSpec(memory_space=pl.ANY)
        sm = pl.BlockSpec(memory_space=pltpu.SMEM)
        dma = pltpu.SemaphoreType.DMA
        dims = (ny, nx, layers, tok, width, heads, hd, seq, experts, local, top, pool_chunks, cap_chunks)
        return pl.pallas_call(
            functools.partial(step_kernel, dims),
            out_shape=jax.ShapeDtypeStruct((tok, width), BF16),
            in_specs=[vm, hb, hb, sm, hb, hb, hb, hb, hb, vm, vm, hb, hb, hb],
            out_specs=vm,
            scratch_shapes=[
                pltpu.VMEM((tok, width), BF16), pltpu.VMEM((tok, width), BF16), pltpu.VMEM((tok, width), BF16), pltpu.VMEM((2 * top, tok), F32),
                pltpu.VMEM((tok, heads, hd), F32), pltpu.VMEM((tok, heads, hd), F32),
                pltpu.VMEM((BLOCK * heads, seq), F32), pltpu.VMEM((BLOCK * heads, hd), F32), pltpu.VMEM((tok, hd), F32), pltpu.VMEM((tok, hd), F32),
                pltpu.VMEM((width, heads * hd), BF16), pltpu.VMEM((width, hd), BF16), pltpu.VMEM((width, hd), BF16),
                pltpu.VMEM((heads * hd, width), BF16), pltpu.VMEM((width, experts), F32),
                pltpu.VMEM((group,) + mine.shape, I32), pltpu.VMEM((local, group, tok), I32),
                pltpu.VMEM((group + pools + 8, tok), I32), pltpu.SMEM((group + pools + 8, tok), I32),
                pltpu.VMEM((group, tok, width), BF16),
                pltpu.VMEM((pools * pool_chunks, CHUNK, width), BF16), pltpu.VMEM((TILE, width), BF16),
                pltpu.VMEM((local * cap_chunks // per, TILE, ff), BF16), pltpu.VMEM((local * cap_chunks, CHUNK, 2 * quarter), BF16),
                pltpu.VMEM((pools, 2 * WINDOW, pool_chunks * CHUNK), BF16),
                pltpu.VMEM((tok * seq, LANES), BF16), pltpu.VMEM((tok * seq, LANES), BF16),
                pltpu.VMEM((8, 3 * tok, 2 * nx * WINDOW), BF16),
                pltpu.VMEM((4, 4, tok, quarter), F32), pltpu.VMEM((4, 4, tok, quarter), F32), pltpu.VMEM((2, 4, 2 * top, tok), F32),
                pltpu.VMEM((local, width, ff), BF16), pltpu.VMEM((local, width, ff), BF16), pltpu.VMEM((local, ff, width), BF16),
                dma((tok // BLOCK,)), dma((tok // BLOCK,)), dma((5,)), dma((3, local)), dma,
                dma((group,)), dma((group,)), dma((128,)), dma((128,)), dma((64,)), dma((64,)), dma((8,)), dma((8,)),
                dma((32,)), dma((32,)), dma((16,)), dma((16,)),
            ],
            compiler_params=pltpu.CompilerParams(vmem_limit_bytes=67043328, collective_id=0, has_side_effects=True),
            name='step',
        )(hidden, k_cache, v_cache, lengths, w_query, w_key, w_value, w_out, w_router, expert_ids, mine, w_gate, w_up, w_down)

    cache_spec = P(None, BATCH_AXES, None, None, None)
    expert_spec = P(None, GROUP_AXES, None, None)
    in_specs = (P(BATCH_AXES, None), cache_spec, cache_spec, P(BATCH_AXES), P(), P(), P(), P(), P(), P(None, BATCH_AXES, None), expert_spec, expert_spec, expert_spec)
    return jax.shard_map(device_step, mesh=mesh, in_specs=in_specs, out_specs=P(BATCH_AXES, None), check_vma=False)
```

```python
import functools

import jax
import jax.numpy as jnp
from jax import lax
from jax.experimental import pallas as pl
from jax.experimental.pallas import tpu as pltpu
from jax.sharding import PartitionSpec as P

EPS = 1e-6
GROUP_AXES = ('pool', 'ep')
BATCH_AXES = ('dp', 'pool', 'ep')
F32 = jnp.float32
BF16 = jnp.bfloat16
I32 = jnp.int32
CHUNK = 16
WINDOW = 64
TILE = 256
LANES = 128
BLOCK = 16
WAVES = 2
MESH = pl.DeviceIdType.MESH
OFFS = (0, -1, 1, 2)
IDX = {0: 0, 1: 1, -1: 2, 2: 3}
BACK = {1: -1, -1: 1, 2: 2}


def rms_norm(wide):
    return (wide * lax.rsqrt(jnp.mean(wide * wide, axis=-1, keepdims=True) + EPS)).astype(BF16)


def dot(a, b):
    return jnp.dot(a, b, preferred_element_type=F32)


def dot_t(a, b):
    return lax.dot_general(a, b, (((1,), (1,)), ((), ())), preferred_element_type=F32)


def split3(w):
    hi = w.astype(BF16)
    rest = w - hi.astype(F32)
    mid = rest.astype(BF16)
    low = (rest - mid.astype(F32)).astype(BF16)
    return hi, mid, low


def iota(shape, axis):
    return lax.broadcasted_iota(I32, shape, axis)


def onehot(cond):
    return jnp.where(cond, 1.0, 0.0).astype(BF16)


def step_kernel(dims, hidden_ref, kc_hbm, vc_hbm, len_ref, wq_hbm, wk_hbm, wv_hbm, wo_hbm, wr_hbm, mine_ref, wg_hbm, wu_hbm, wd_hbm,
                x_ref,
                xcur, abuf, ubuf0, gs, idc, slotc, q3, o3, sbuf, nbuf, kn3, vn3, wq, wk, wv, wo, wr,
                idsbuf, keys, tabv, tab, ubuf, xg, xt, act, yq, pick, rbuf, vbuf, gmat, part, final, gsbuf, wg, wu, wd,
                ksem, vsem, asem, wsem, tsem, id_send, id_recv, ag_send, ag_recv, dd_send, dd_recv, gs_send, gs_recv,
                p1_send, p1_recv, p2_send, p2_recv):
    ny, nx, layers, tok, width, heads, hd, seq, experts, local, top, pool_chunks, cap_chunks = dims
    pools = ny * nx
    group = 2 * pools
    pool_rows = pool_chunks * CHUNK
    span = tok // WAVES
    half = span // 2
    steps = width // (2 * LANES)
    per = TILE // CHUNK
    per_expert = cap_chunks // per
    slots = 2 * nx * WINDOW
    y = lax.axis_index('pool')
    ep = lax.axis_index('ep')
    x = ep // 2
    core = lax.rem(ep, 2)
    other = 1 - core
    me = y * (2 * nx) + ep

    def at(dx, dy):
        return lax.rem(x + dx + nx, nx), lax.rem(y + dy + ny, ny)

    def dev(dx, dy, c):
        px, py = at(dx, dy)
        return {'pool': py, 'ep': px * 2 + c}

    def number(dx, dy, c):
        px, py = at(dx, dy)
        return py * (2 * nx) + px * 2 + c

    def axes(h, first, second):
        return (first, second) if h == 0 else (second, first)

    def peer(d):
        to = lax.rem(me + d, group)
        return {'pool': to // (2 * nx), 'ep': lax.rem(to, 2 * nx)}

    def remote(src, dst, send, recv, device):
        return pltpu.make_async_remote_copy(src_ref=src, dst_ref=dst, send_sem=send, recv_sem=recv, device_id=device, device_id_type=MESH)

    def att_copies(layer):
        return [pltpu.make_async_copy(src.at[layer], dst, asem.at[i])
                for i, (src, dst) in enumerate(((wq_hbm, wq), (wk_hbm, wk), (wv_hbm, wv), (wo_hbm, wo), (wr_hbm, wr)))]

    def expert_copies(layer):
        return [pltpu.make_async_copy(src.at[layer, e], dst.at[e], wsem.at[i, e])
                for i, (src, dst) in enumerate(((wg_hbm, wg), (wu_hbm, wu), (wd_hbm, wd))) for e in range(local)]

    def kv_copies(layer, b):
        rows = pl.ds(b * (BLOCK * seq), BLOCK * seq)
        return (pltpu.make_async_copy(kc_hbm.at[layer, rows], rbuf.at[rows], ksem.at[b]),
                pltpu.make_async_copy(vc_hbm.at[layer, rows], vbuf.at[rows], vsem.at[b]))

    def id_copy(d):
        return remote(mine_ref, idsbuf.at[me], id_send.at[d], id_recv.at[d], peer(d))

    def piece(w, h, r, q, p=None):
        if q == 0:
            step = 1 if (r == -1 or (r == 2 and p == 0)) else -1
            own = (0, 0) if r in (1, -1) else (-step, 0)
            to = (step, 0)
        else:
            step = 1 if (q == -1 or (q == 2 and p == 0)) else -1
            own = (r, 0) if q in (1, -1) else (r, -step)
            to = (0, step)
        first = w * span + h * half
        rows = pl.ds(first, half) if p is None else pl.ds(first + p * (half // 2), half // 2)
        owner = number(*axes(h, *own), core)
        src = ubuf0.at[rows] if own == (0, 0) else ubuf.at[owner, rows]
        sem = (((w * 2 + h) * 4 + IDX[r]) * 4 + IDX[q]) * 2 + (p or 0)
        return remote(src, ubuf.at[owner, rows], ag_send.at[sem], ag_recv.at[sem], dev(*axes(h, *to), core))

    def across(w, h, r, q):
        rows = pl.ds(w * span + h * half, half)
        owner = number(*axes(h, r, q), core)
        src = ubuf0.at[rows] if (r, q) == (0, 0) else ubuf.at[owner, rows]
        sem = ((w * 2 + h) * 4 + IDX[r]) * 4 + IDX[q]
        return remote(src, ubuf.at[owner, rows], dd_send.at[sem], dd_recv.at[sem], dev(0, 0, other))

    def gate_copy(h, q):
        back = IDX[BACK[q]]
        sem = h * 4 + back
        return remote(gs, gsbuf.at[h, back], gs_send.at[sem], gs_recv.at[sem], dev(*axes(h, 0, q), core))

    def window_row(n, one, c, two=0):
        return ((n * nx + one) * 2 + c) * (ny * WINDOW) + two * WINDOW

    def first_copy(h, w, r, flip):
        n = h * steps + w
        c = other if flip else core
        size = ny * WINDOW
        src = pl.ds(pl.multiple_of(window_row(n, at(r, r)[h], c), size), size)
        dst = pl.ds(pl.multiple_of(window_row(n, (x, y)[h], core), size), size)
        sem = (n * 4 + IDX[r]) * 2 + flip
        return remote(rbuf.at[src], vbuf.at[dst], p1_send.at[sem], p1_recv.at[sem], dev(*axes(h, r, 0), c))

    def second_copy(h, w, q):
        n = h * steps + w
        sem = n * 4 + IDX[q]
        return remote(part.at[n, IDX[q]], final.at[n, IDX[q]], p2_send.at[sem], p2_recv.at[sem], dev(*axes(h, 0, q), core))

    for cp in att_copies(0):
        cp.start()
    barrier = pltpu.get_barrier_semaphore()
    for d in range(1, group):
        pl.semaphore_signal(barrier, inc=1, device_id=peer(d), device_id_type=MESH)
    pl.semaphore_wait(barrier, group - 1)
    for d in range(1, group):
        id_copy(d).start()
    idsbuf[me] = mine_ref[...]
    xcur[...] = hidden_ref[...]
    scale = hd ** -0.5
    lane = iota((heads, seq), 1)

    tab_y0 = group
    tab_x0 = group + pools

    def own_slots(layer):
        e_iota = iota((tok, experts), 1)
        before = onehot(iota((tok, tok), 1) < iota((tok, tok), 0))
        e_row = iota((experts, experts), 0)
        e_col = iota((experts, experts), 1)
        same = onehot((e_row < e_col) & (e_row // local == e_col // local))
        ids = jnp.concatenate([mine_ref[layer].astype(F32), jnp.zeros((LANES - top, tok), F32)], axis=0)
        ids = jnp.transpose(ids).astype(I32)
        idc[...] = ids
        hits = [ids[:, k:k + 1] == e_iota for k in range(top)]
        chosen = hits[0]
        for k in range(1, top):
            chosen = chosen | hits[k]
        chosen = jnp.where(chosen, 1.0, 0.0)
        rank = dot(before, chosen.astype(BF16))
        count = jnp.sum(chosen, axis=0, keepdims=True)
        start = dot(jnp.broadcast_to(count, (8, experts)).astype(BF16), same)[0:1]
        slot_full = rank + start + ((e_iota // local) * WINDOW).astype(F32)
        for k in range(top):
            slotc[:, k:k + 1] = jnp.sum(jnp.where(hits[k], slot_full, 0.0), axis=1, keepdims=True)

    def tables(layer):
        before_tok = onehot(iota((tok, tok), 0) < iota((tok, tok), 1))
        before_pool = onehot(iota((pools, pools), 1) < iota((pools, pools), 0))
        pair_of = onehot(iota((pools, group), 1) // 2 == iota((pools, group), 0))
        spread = onehot(iota((group, pools), 0) // 2 == iota((group, pools), 1))
        prev = onehot((iota((group, group), 1) + 1 == iota((group, group), 0)) & (iota((group, group), 0) % 2 == 1))
        lane_p = iota((pools, tok), 1)
        pool_id = iota((pools, tok), 0)
        lane_s = iota((group, tok), 1)
        off = jnp.zeros((pools, tok), I32)
        lo = jnp.zeros((group, tok), I32)
        tab_y = jnp.zeros((pools, tok), I32)
        tab_s = jnp.zeros((group, tok), I32)
        rows_x = []
        for e in range(local):
            target = me * local + e
            hit = idsbuf[:, layer, 0, :] == target
            for k in range(1, top):
                hit = hit | (idsbuf[:, layer, k, :] == target)
            hitb = onehot(hit)
            rank = dot(hitb, before_tok).astype(I32)
            count = jnp.broadcast_to(jnp.sum(jnp.where(hit, 1.0, 0.0), axis=1, keepdims=True), (group, tok))
            countb = count.astype(BF16)
            count = count.astype(I32)
            amount = dot(pair_of, countb).astype(I32)
            chunks = lax.shift_right_logical(amount + (CHUNK - 1), 4)
            base = dot(before_pool, chunks.astype(F32).astype(BF16)).astype(I32)
            shift = dot(spread, (off * CHUNK).astype(F32).astype(BF16)).astype(I32) + dot(prev, countb).astype(I32)
            keys[e] = jnp.where(hit, rank + shift, -1)
            rows_x.append(jnp.sum(jnp.where((lane_p >= base) & (lane_p < base + chunks), pool_id * pool_chunks + off + lane_p - base, 0).astype(F32),
                                  axis=0, keepdims=True))
            tab_y = jnp.where((lane_p >= off) & (lane_p < off + chunks), e * cap_chunks + base + lane_p - off, tab_y)
            tab_s = jnp.where(lane_s == e, lo, tab_s)
            tab_s = jnp.where(lane_s == local + e, lo + count, tab_s)
            tab_s = jnp.where(lane_s == 2 * local + e, shift - lo, tab_s)
            off = off + chunks
            lo = lo + count
        tabv[0:group, :] = tab_s
        tabv[group:group + pools, :] = jnp.clip(tab_y, 0, local * cap_chunks - 1)
        rows_x.append(jnp.zeros((8 - local, tok), F32))
        tabv[tab_x0:tab_x0 + 8, :] = jnp.clip(jnp.concatenate(rows_x, axis=0).astype(I32), 0, pools * pool_chunks - 1)
        tab_copy = pltpu.make_async_copy(tabv, tab, tsem)
        tab_copy.start()
        tab_copy.wait()
        jrow = iota((WINDOW, pool_rows), 0)
        diff = iota((WINDOW, pool_rows), 1) - jrow

        def choose(chip, c2):
            halves = []
            for par in range(2):
                hit = None
                for e in range(local):
                    low_ = tab[2 * chip + par, e]
                    high_ = tab[2 * chip + par, local + e]
                    delta = tab[2 * chip + par, 2 * local + e]
                    this = (diff == delta) & (jrow >= low_) & (jrow < high_)
                    hit = this if hit is None else hit | this
                halves.append(onehot(hit))
            pick[chip] = jnp.concatenate(halves, axis=0)
            return c2

        lax.fori_loop(0, pools, choose, 0, unroll=2)

    own_slots(0)

    def layer_body(layer, carry):
        for b in range(tok // BLOCK):
            for cp in kv_copies(layer, b):
                cp.start()
        for cp in expert_copies(layer):
            cp.start()
        normed = rms_norm(xcur[...].astype(F32))
        for cp in att_copies(layer)[:3]:
            cp.wait()
        kn3[...] = dot(normed, wk[...]).astype(BF16).astype(F32)
        vn3[...] = dot(normed, wv[...]).astype(BF16).astype(F32)
        for h in range(heads):
            if h % 2 == 0:
                pair = dot(normed, wq[:, h * hd:(h + 2) * hd])
            q3[:, h, :] = pair[:, (h % 2) * hd:(h % 2 + 1) * hd].astype(BF16).astype(F32)

        def scores(b, part_):
            kv_copies(layer, b)[0].wait()
            for j in range(BLOCK):
                t = b * BLOCK + j
                q = q3[t]
                s = dot_t(q.astype(BF16), rbuf[pl.ds(t * seq, seq), :]) * scale
                sbuf[part_, j * heads:(j + 1) * heads, :] = jnp.where(lane < len_ref[t], s, -jnp.inf)
                nbuf[part_, j * heads:(j + 1) * heads, :] = q * kn3[pl.ds(t, 1), :]

        def weigh(b, part_):
            s = sbuf[part_]
            sn = jnp.sum(nbuf[part_], axis=1, keepdims=True) * scale
            peak = jnp.maximum(jnp.max(s, axis=1, keepdims=True), sn)
            p = jnp.exp(s - peak)
            pn = jnp.exp(sn - peak)
            inv = 1.0 / (jnp.sum(p, axis=1, keepdims=True) + pn)
            pb = (p * inv).astype(BF16)
            pnb = (pn * inv).astype(BF16).astype(F32)
            kv_copies(layer, b)[1].wait()
            for j in range(BLOCK):
                t = b * BLOCK + j
                rows = slice(j * heads, (j + 1) * heads)
                o = dot(pb[rows], vbuf[pl.ds(t * seq, seq), :]) + pnb[rows] * vn3[pl.ds(t, 1), :]
                o3[t] = o.astype(BF16).astype(F32)

        def block(i, c2):
            scores(2 * i, 0)
            scores(2 * i + 1, 1)
            weigh(2 * i, 0)
            weigh(2 * i + 1, 1)
            return c2

        def project(w):
            rows = slice(w * span, (w + 1) * span)
            mixed = jnp.concatenate([o3[rows, h, :].astype(BF16) for h in range(heads)], axis=1)
            a = (xcur[rows].astype(F32) + dot(mixed, wo[...])).astype(BF16)
            abuf[rows] = a
            ubuf0[rows] = rms_norm(a.astype(F32))

        started = []

        def go(fn, *args):
            fn(*args).start()
            started.append((fn, args))

        have = set()
        done = set()
        prow = iota((pool_rows, tok), 0)

        def gather(dx, dy):
            px, py = at(dx, dy)
            chip = py * nx + px
            for w in range(WAVES):
                across(w, 0, dx, dy).wait_recv()
                across(w, 1, dy, dx).wait_recv()
            halves = []
            for par in range(2):
                hit = None
                for e in range(local):
                    this = prow == keys[e, pl.ds(2 * chip + par, 1), :]
                    hit = this if hit is None else hit | this
                halves.append(onehot(hit))
            rows = ubuf[pl.ds(2 * chip, 2)].reshape(2 * tok, width)
            xg[pl.ds(chip * pool_chunks, pool_chunks)] = dot(jnp.concatenate(halves, axis=1), rows).astype(BF16).reshape(pool_chunks, CHUNK, width)

        def ready(limit):
            for dy in OFFS:
                for dx in OFFS:
                    if limit and (dx, dy) not in done and all((w, 0, dx, dy) in have and (w, 1, dy, dx) in have for w in range(WAVES)):
                        done.add((dx, dy))
                        gather(dx, dy)
                        limit -= 1

        def s0(w):
            for h in (0, 1):
                go(piece, w, h, -1, 0)
                go(piece, w, h, 1, 0)
            for h in (0, 1):
                go(piece, w, h, 0, -1)
                go(piece, w, h, 0, 1)
                go(across, w, h, 0, 0)
                have.add((w, h, 0, 0))

        def s2(w):
            for r, p in ((-1, 0), (1, 1)):
                for h in (0, 1):
                    piece(w, h, r, 0).wait_recv()
                    go(piece, w, h, 2, 0, p)
                    go(piece, w, h, r, -1)
                    go(piece, w, h, r, 1)
                    go(across, w, h, r, 0)
                    have.add((w, h, r, 0))

        def s3(w):
            for h in (0, 1):
                piece(w, h, 2, 0, 0).wait_recv()
                piece(w, h, 2, 0, 1).wait_recv()
                go(piece, w, h, 2, -1)
                go(piece, w, h, 2, 1)
                go(across, w, h, 2, 0)
                have.add((w, h, 2, 0))

        def s4(w, r):
            for q, p in ((-1, 0), (1, 1)):
                for h in (0, 1):
                    piece(w, h, r, q).wait_recv()
                    go(piece, w, h, r, 2, p)
                    go(across, w, h, r, q)
                    have.add((w, h, r, q))

        def s5(w, r):
            for h in (0, 1):
                piece(w, h, r, 2, 0).wait_recv()
                piece(w, h, r, 2, 1).wait_recv()
                go(across, w, h, r, 2)
                have.add((w, h, r, 2))

        blocks = span // (2 * BLOCK)
        lax.fori_loop(0, blocks, block, 0)
        att_copies(layer)[3].wait()
        project(0)
        s0(0)
        lax.fori_loop(blocks, 2 * blocks - 1, block, 0)
        s2(0)
        lax.fori_loop(2 * blocks - 1, 2 * blocks, block, 0)
        s4(0, 0)
        project(1)
        s0(1)
        s3(0)

        att_copies(layer)[4].wait()
        hi, mid, low = split3(wr[...])
        u = ubuf0[...]
        logits = dot(u, hi) + dot(u, mid) + dot(u, low)

        @pl.when(layer + 1 < layers)
        def _():
            for cp in att_copies(layer + 1):
                cp.start()

        e_iota = iota((tok, experts), 1)
        hits = [idc[:, k:k + 1] == e_iota for k in range(top)]
        picked = [jnp.sum(jnp.where(hit, logits, 0.0), axis=1, keepdims=True) for hit in hits]
        peak = picked[0]
        for k in range(1, top):
            peak = jnp.maximum(peak, picked[k])
        ex = [jnp.exp(v - peak) for v in picked]
        total = ex[0]
        for k in range(1, top):
            total = total + ex[k]
        columns = [v / total for v in ex] + [slotc[...]]
        columns.append(jnp.zeros((tok, LANES - 2 * top), F32))
        gs[...] = jnp.transpose(jnp.concatenate(columns, axis=1))[:2 * top]
        ubuf[me] = u
        for h in (0, 1):
            for q in OFFS[1:]:
                go(gate_copy, h, q)
        s4(0, -1)
        s4(0, 1)
        s2(1)

        @pl.when(layer == 0)
        def _():
            for d in range(1, group):
                id_copy(d).wait()
            tables(0)

        s4(0, 2)
        s3(1)
        for r in OFFS:
            s5(0, r)
        ready(1)
        s4(1, 0)
        ready(2)

        srow = iota((slots, tok), 0)

        def gates(h):
            for q in OFFS:
                if q:
                    gate_copy(h, BACK[q]).wait_recv()
                    table = gsbuf[h, IDX[q]]
                else:
                    table = gs[...]
                slot = table[top:2 * top].astype(I32)
                if h == 0:
                    rel = slot - y * slots
                else:
                    source = lax.shift_right_logical(slot, 6)
                    sx = lax.shift_right_logical(source, 1) & (nx - 1)
                    sy = source // (2 * nx)
                    rel = jnp.where(sx == x, (sy * 2 + (source & 1)) * WINDOW + (slot & (WINDOW - 1)), -1)
                g = jnp.zeros((slots, tok), F32)
                for k in range(top):
                    g = jnp.where(srow == rel[k:k + 1], table[k:k + 1], g)
                for i, v in enumerate(split3(jnp.transpose(g))):
                    gmat[h * 4 + IDX[q], i * tok:(i + 1) * tok, :] = v

        s4(1, -1)
        s4(1, 1)
        ready(2)
        s4(1, 2)
        ready(3)
        s5(1, 0)
        ready(2)
        s5(1, -1)
        s5(1, 1)
        ready(4)
        s5(1, 2)
        ready(pools)

        for cp in expert_copies(layer):
            cp.wait()

        def tile(i, c2):
            e = i // per_expert
            first_chunk = (i % per_expert) * per
            for j in range(per):
                xt[j * CHUNK:(j + 1) * CHUNK, :] = xg[tab[tab_x0 + e, first_chunk + j]]
            rows_in = xt[...]
            first = dot(rows_in, wg[e])
            second = dot(rows_in, wu[e])
            act[i] = (first * (1.0 / (1.0 + jnp.exp(-first))) * second).astype(BF16)
            return c2

        lax.fori_loop(0, local * per_expert, tile, 0)
        for fn, args in started:
            fn(*args).wait_send()
        started.clear()

        firsts = [(2, 0), (2, 1), (1, 0), (-1, 0), (1, 1), (-1, 1), (0, 1)]
        wide = 2
        for w in range(steps):
            if w % wide == 0:
                def down(i, c2):
                    out = dot(act[i], wd[i // per_expert, :, w * 2 * LANES:(w + wide) * 2 * LANES])
                    yq[pl.ds(i * per, per)] = out.astype(BF16).reshape(per, CHUNK, wide * 2 * LANES)
                    return c2

                lax.fori_loop(0, local * per_expert, down, 0, unroll=2)

            def window(chip, c2):
                inside = slice((w % wide) * 2 * LANES, (w % wide + 1) * 2 * LANES)
                rows = jnp.concatenate([yq[tab[tab_y0 + chip, i], :, inside] for i in range(pool_chunks)], axis=0)
                out = dot(pick[chip], rows).astype(BF16)
                cy = chip // nx
                cx = chip % nx
                for h in (0, 1):
                    one, two = axes(h, cx, cy)
                    for par in range(2):
                        row = pl.multiple_of(window_row(h * steps + w, one, par, two), WINDOW)
                        rbuf[pl.ds(row, WINDOW), :] = out[par * WINDOW:(par + 1) * WINDOW, h * LANES:(h + 1) * LANES]
                return c2

            lax.fori_loop(0, pools, window, 0, unroll=4)
            for r, flip in firsts:
                for h in (0, 1):
                    go(first_copy, h, w, r, flip)
            for h in (0, 1):
                size = ny * WINDOW
                own = pl.ds(pl.multiple_of(window_row(h * steps + w, (x, y)[h], core), size), size)
                vbuf[own, :] = rbuf[own, :]

        def merge(h, ws):
            for w in ws:
                for r, flip in firsts:
                    first_copy(h, w, r, flip).wait_recv()
            for q in (2, 1, -1, 0):
                two = at(q, q)[1 - h]
                rows = []
                for s in range(2 * nx):
                    pieces = [vbuf[pl.ds(pl.multiple_of(window_row(h * steps + w, s // 2, s % 2, two), WINDOW), WINDOW), :] for w in ws]
                    rows.append(jnp.concatenate(pieces, axis=1))
                parts = dot(gmat[h * 4 + IDX[q]], jnp.concatenate(rows, axis=0))
                total = parts[0:tok] + parts[tok:2 * tok] + parts[2 * tok:3 * tok]
                for i, w in enumerate(ws):
                    part[h * steps + w, IDX[q]] = total[:, i * LANES:(i + 1) * LANES]
                if q:
                    for w in ws:
                        go(second_copy, h, w, q)

        for h in (0, 1):
            gates(h)
        for h in (0, 1):
            merge(h, (0, 1))

        @pl.when(layer + 1 < layers)
        def _():
            own_slots(layer + 1)
            tables(layer + 1)

        for w in range(2, steps):
            for h in (0, 1):
                merge(h, (w,))
        for w in range(steps):
            for h in (0, 1):
                n = h * steps + w
                where = slice((w * 2 + h) * LANES, (w * 2 + h + 1) * LANES)
                for q in OFFS[1:]:
                    second_copy(h, w, q).wait_recv()
                total = (part[n, 0] + final[n, 1]) + (final[n, 2] + final[n, 3])
                xcur[:, where] = (abuf[:, where].astype(F32) + total).astype(BF16)
        for fn, args in started:
            fn(*args).wait_send()
        return carry

    lax.fori_loop(0, layers, layer_body, 0)
    x_ref[...] = xcur[...]


def solution(mesh):
    ny, nx = mesh.shape['pool'], mesh.shape['ep'] // 2

    def device_step(hidden, k_cache, v_cache, lengths, w_query, w_key, w_value, w_out, w_router, expert_ids, w_gate, w_up, w_down):
        tok, width = hidden.shape
        layers, _, top = expert_ids.shape
        seq, hd = k_cache.shape[2], k_cache.shape[4]
        heads = w_query.shape[2] // hd
        experts = w_router.shape[2]
        local, ff = w_gate.shape[1], w_gate.shape[3]
        pools = nx * ny
        group = 2 * pools
        k_cache = k_cache.reshape(layers, tok * seq, hd)
        v_cache = v_cache.reshape(layers, tok * seq, hd)
        mine = jnp.swapaxes(expert_ids, 1, 2)
        pool_chunks = (2 * (WINDOW - 1) + local * (CHUNK - 1)) // CHUNK
        most = 2 * group * tok * top // (group * local)
        per = TILE // CHUNK
        cap_chunks = pl.cdiv((most + pools * (CHUNK - 1)) // CHUNK, per) * per
        steps = width // (2 * LANES)
        vm = pl.BlockSpec(memory_space=pltpu.VMEM)
        hb = pl.BlockSpec(memory_space=pl.ANY)
        sm = pl.BlockSpec(memory_space=pltpu.SMEM)
        dma = pltpu.SemaphoreType.DMA
        dims = (ny, nx, layers, tok, width, heads, hd, seq, experts, local, top, pool_chunks, cap_chunks)
        return pl.pallas_call(
            functools.partial(step_kernel, dims),
            out_shape=jax.ShapeDtypeStruct((tok, width), BF16),
            in_specs=[vm, hb, hb, sm, hb, hb, hb, hb, hb, vm, hb, hb, hb],
            out_specs=vm,
            scratch_shapes=[
                pltpu.VMEM((tok, width), BF16), pltpu.VMEM((tok, width), BF16), pltpu.VMEM((tok, width), BF16), pltpu.VMEM((2 * top, tok), F32),
                pltpu.VMEM((tok, LANES), I32), pltpu.VMEM((tok, top), F32),
                pltpu.VMEM((tok, heads, hd), F32), pltpu.VMEM((tok, heads, hd), F32),
                pltpu.VMEM((2, BLOCK * heads, seq), F32), pltpu.VMEM((2, BLOCK * heads, hd), F32), pltpu.VMEM((tok, hd), F32), pltpu.VMEM((tok, hd), F32),
                pltpu.VMEM((width, heads * hd), BF16), pltpu.VMEM((width, hd), BF16), pltpu.VMEM((width, hd), BF16),
                pltpu.VMEM((heads * hd, width), BF16), pltpu.VMEM((width, experts), F32),
                pltpu.VMEM((group,) + mine.shape, I32), pltpu.VMEM((local, group, tok), I32),
                pltpu.VMEM((group + pools + 8, tok), I32), pltpu.SMEM((group + pools + 8, tok), I32),
                pltpu.VMEM((group, tok, width), BF16),
                pltpu.VMEM((pools * pool_chunks, CHUNK, width), BF16), pltpu.VMEM((TILE, width), BF16),
                pltpu.VMEM((local * cap_chunks // per, TILE, ff), BF16), pltpu.VMEM((local * cap_chunks, CHUNK, 4 * LANES), BF16),
                pltpu.VMEM((pools, 2 * WINDOW, pool_chunks * CHUNK), BF16),
                pltpu.VMEM((tok * seq, LANES), BF16), pltpu.VMEM((tok * seq, LANES), BF16),
                pltpu.VMEM((8, 3 * tok, 2 * nx * WINDOW), BF16),
                pltpu.VMEM((2 * steps, 4, tok, LANES), F32), pltpu.VMEM((2 * steps, 4, tok, LANES), F32), pltpu.VMEM((2, 4, 2 * top, tok), F32),
                pltpu.VMEM((local, width, ff), BF16), pltpu.VMEM((local, width, ff), BF16), pltpu.VMEM((local, ff, width), BF16),
                dma((tok // BLOCK,)), dma((tok // BLOCK,)), dma((5,)), dma((3, local)), dma,
                dma((group,)), dma((group,)), dma((128,)), dma((128,)), dma((64,)), dma((64,)), dma((8,)), dma((8,)),
                dma((16 * steps,)), dma((16 * steps,)), dma((8 * steps,)), dma((8 * steps,)),
            ],
            compiler_params=pltpu.CompilerParams(vmem_limit_bytes=67043328, collective_id=0, has_side_effects=True),
            name='step',
        )(hidden, k_cache, v_cache, lengths, w_query, w_key, w_value, w_out, w_router, mine, w_gate, w_up, w_down)

    cache_spec = P(None, BATCH_AXES, None, None, None)
    expert_spec = P(None, GROUP_AXES, None, None)
    in_specs = (P(BATCH_AXES, None), cache_spec, cache_spec, P(BATCH_AXES), P(), P(), P(), P(), P(), P(None, BATCH_AXES, None), expert_spec, expert_spec, expert_spec)
    return jax.shard_map(device_step, mesh=mesh, in_specs=in_specs, out_specs=P(BATCH_AXES, None), check_vma=False)
```

```python
import functools

import jax
import jax.numpy as jnp
from jax import lax
from jax.experimental import pallas as pl
from jax.experimental.pallas import tpu as pltpu
from jax.sharding import PartitionSpec as P

EPS = 1e-6
GROUP_AXES = ('pool', 'ep')
BATCH_AXES = ('dp', 'pool', 'ep')
F32 = jnp.float32
BF16 = jnp.bfloat16
I32 = jnp.int32
CHUNK = 16
WINDOW = 64
TILE = 768
LANES = 128
BLOCK = 16
WAVES = 2
MESH = pl.DeviceIdType.MESH
OFFS = (0, -1, 1, 2)
IDX = {0: 0, 1: 1, -1: 2, 2: 3}
BACK = {1: -1, -1: 1, 2: 2}
NEAR = OFFS[1:3]
NEXT = OFFS[1:]
FAR = OFFS[-1]
BOTH = range(2)
ROWS, COLS = BOTH


def rms_norm(wide):
    return (wide * lax.rsqrt(jnp.mean(wide * wide, axis=-1, keepdims=True) + EPS)).astype(BF16)


def dot(a, b):
    return jnp.dot(a, b, preferred_element_type=F32)


def dot_t(a, b):
    return lax.dot_general(a, b, (((1,), (1,)), ((), ())), preferred_element_type=F32)


def split3(w):
    hi = w.astype(BF16)
    rest = w - hi.astype(F32)
    mid = rest.astype(BF16)
    low = (rest - mid.astype(F32)).astype(BF16)
    return hi, mid, low


def iota(shape, axis):
    return lax.broadcasted_iota(I32, shape, axis)


def ones(cond):
    return jnp.where(cond, 1.0, 0.0)


def onehot(cond):
    return ones(cond).astype(BF16)


def zeros(*shape, dtype=F32):
    return jnp.zeros(shape, dtype)


def row_max(v):
    return jnp.max(v, axis=1, keepdims=True)


def row_sum(v):
    return jnp.sum(v, axis=1, keepdims=True)


def sigmoid(v):
    return 1.0 / (1.0 + jnp.exp(-v))


def down_iota(shape):
    return iota(shape, 0)


def across_iota(shape):
    return iota(shape, 1)


def fold(fn, values):
    return functools.reduce(fn, values)


def vmem(*shape, dtype=BF16):
    return pltpu.VMEM(shape, dtype)


def step_kernel(dims, hidden_ref, kc_hbm, vc_hbm, len_ref, wq_hbm, wk_hbm, wv_hbm, wo_hbm, wr_hbm, mine_ref, wg_hbm, wu_hbm, wd_hbm,
                x_ref,
                xcur, abuf, ubuf0, gs, idc, slotc, q3, o3, sbuf, nbuf, kn3, vn3, wq, wk, wv, wo, wr,
                idsbuf, keys, tabv, tab, ubuf, xg, xt, act, yq, pick, rbuf, vbuf, gmat, part, final, gsbuf, wg, wu, wd,
                ksem, vsem, asem, wsem, tsem, id_send, id_recv, ag_send, ag_recv, dd_send, dd_recv, gs_send, gs_recv,
                p1_send, p1_recv, p2_send, p2_recv):
    ny, nx, layers, tok, width, heads, hd, seq, experts, local, top, pool_chunks, cap_chunks = dims
    pools = ny * nx
    group = 2 * pools
    pair_lanes = 2 * LANES
    pool_rows = pool_chunks * CHUNK
    span = tok // WAVES
    half = span // 2
    steps = width // (2 * LANES)
    per = TILE // CHUNK
    per_expert = cap_chunks // per
    slots = 2 * nx * WINDOW
    y = lax.axis_index('pool')
    ep = lax.axis_index('ep')
    x = ep // 2
    core = lax.rem(ep, 2)
    other = 1 - core
    me = y * (2 * nx) + ep

    def at(dx, dy):
        return lax.rem(x + dx + nx, nx), lax.rem(y + dy + ny, ny)

    def dev(dx, dy, c):
        px, py = at(dx, dy)
        return {'pool': py, 'ep': px * 2 + c}

    def number(dx, dy, c):
        px, py = at(dx, dy)
        return py * (2 * nx) + px * 2 + c

    def axes(h, first, second):
        return (first, second) if h == 0 else (second, first)

    def peer(d):
        to = lax.rem(me + d, group)
        return {'pool': to // (2 * nx), 'ep': lax.rem(to, 2 * nx)}

    def remote(src, dst, send, recv, device):
        return pltpu.make_async_remote_copy(src_ref=src, dst_ref=dst, send_sem=send, recv_sem=recv, device_id=device, device_id_type=MESH)

    def att_copies(layer):
        return [pltpu.make_async_copy(src.at[layer], dst, asem.at[i])
                for i, (src, dst) in enumerate(((wq_hbm, wq), (wk_hbm, wk), (wv_hbm, wv), (wo_hbm, wo), (wr_hbm, wr)))]

    def expert_copies(layer):
        return [pltpu.make_async_copy(src.at[layer, e], dst.at[e], wsem.at[i, e])
                for i, (src, dst) in enumerate(((wg_hbm, wg), (wu_hbm, wu), (wd_hbm, wd))) for e in range(local)]

    def kv_copies(layer, b):
        rows = pl.ds(b * (BLOCK * seq), BLOCK * seq)
        return (pltpu.make_async_copy(kc_hbm.at[layer, rows], rbuf.at[rows], ksem.at[b]),
                pltpu.make_async_copy(vc_hbm.at[layer, rows], vbuf.at[rows], vsem.at[b]))

    def id_copy(d):
        return remote(mine_ref, idsbuf.at[me], id_send.at[d], id_recv.at[d], peer(d))

    def piece(w, h, r, q, p=None):
        if q == 0:
            step = 1 if (r == -1 or (r == 2 and p == 0)) else -1
            own = (0, 0) if r in (1, -1) else (-step, 0)
            to = (step, 0)
        else:
            step = 1 if (q == -1 or (q == 2 and p == 0)) else -1
            own = (r, 0) if q in (1, -1) else (r, -step)
            to = (0, step)
        first = w * span + h * half
        rows = pl.ds(first, half) if p is None else pl.ds(first + p * (half // 2), half // 2)
        owner = number(*axes(h, *own), core)
        src = ubuf0.at[rows] if own == (0, 0) else ubuf.at[owner, rows]
        sem = (((w * 2 + h) * 4 + IDX[r]) * 4 + IDX[q]) * 2 + (p or 0)
        return remote(src, ubuf.at[owner, rows], ag_send.at[sem], ag_recv.at[sem], dev(*axes(h, *to), core))

    def across(w, h, r, q):
        rows = pl.ds(w * span + h * half, half)
        owner = number(*axes(h, r, q), core)
        src = ubuf0.at[rows] if (r, q) == (0, 0) else ubuf.at[owner, rows]
        sem = ((w * 2 + h) * 4 + IDX[r]) * 4 + IDX[q]
        return remote(src, ubuf.at[owner, rows], dd_send.at[sem], dd_recv.at[sem], dev(0, 0, other))

    def gate_copy(h, q):
        back = IDX[BACK[q]]
        sem = h * 4 + back
        return remote(gs, gsbuf.at[h, back], gs_send.at[sem], gs_recv.at[sem], dev(*axes(h, 0, q), core))

    def window_row(n, one, c, two=0):
        return ((n * nx + one) * 2 + c) * (ny * WINDOW) + two * WINDOW

    def first_copy(h, w, r, flip):
        n = h * steps + w
        c = other if flip else core
        size = ny * WINDOW
        src = pl.ds(pl.multiple_of(window_row(n, at(r, r)[h], c), size), size)
        dst = pl.ds(pl.multiple_of(window_row(n, (x, y)[h], core), size), size)
        sem = (n * 4 + IDX[r]) * 2 + flip
        return remote(rbuf.at[src], vbuf.at[dst], p1_send.at[sem], p1_recv.at[sem], dev(*axes(h, r, 0), c))

    def second_copy(h, w, q):
        n = h * steps + w
        sem = n * 4 + IDX[q]
        return remote(part.at[n, IDX[q]], final.at[n, IDX[q]], p2_send.at[sem], p2_recv.at[sem], dev(*axes(h, 0, q), core))

    for cp in att_copies(0):
        cp.start()
    barrier = pltpu.get_barrier_semaphore()
    for d in range(1, group):
        pl.semaphore_signal(barrier, inc=1, device_id=peer(d), device_id_type=MESH)
    pl.semaphore_wait(barrier, group - 1)
    for d in range(1, group):
        id_copy(d).start()
    idsbuf[me] = mine_ref[...]
    xcur[...] = hidden_ref[...]
    scale = hd ** -0.5
    lane = across_iota((heads, seq))

    tab_y0 = group
    tab_x0 = group + pools

    def own_slots(layer):
        e_iota = across_iota((tok, experts))
        before = onehot(across_iota((tok, tok)) < down_iota((tok, tok)))
        e_row = down_iota((experts, experts))
        e_col = across_iota((experts, experts))
        same = onehot((e_row < e_col) & (e_row // local == e_col // local))
        ids = jnp.concatenate([mine_ref[layer].astype(F32), zeros(LANES - top, tok)], axis=0)
        ids = jnp.transpose(ids).astype(I32)
        idc[...] = ids
        hits = [ids[:, k:k + 1] == e_iota for k in range(top)]
        chosen = fold(jnp.logical_or, hits)
        chosen = ones(chosen)
        rank = dot(before, chosen.astype(BF16))
        count = jnp.sum(chosen, axis=0, keepdims=True)
        start = dot(jnp.broadcast_to(count, (8, experts)).astype(BF16), same)[0:1]
        slot_full = rank + start + ((e_iota // local) * WINDOW).astype(F32)
        for k in range(top):
            slotc[:, k:k + 1] = row_sum(jnp.where(hits[k], slot_full, 0.0))

    def tables(layer):
        before_tok = onehot(down_iota((tok, tok)) < across_iota((tok, tok)))
        before_pool = onehot(across_iota((pools, pools)) < down_iota((pools, pools)))
        pair_of = onehot(across_iota((pools, group)) // 2 == down_iota((pools, group)))
        spread = onehot(down_iota((group, pools)) // 2 == across_iota((group, pools)))
        prev = onehot((across_iota((group, group)) + 1 == down_iota((group, group))) & (down_iota((group, group)) % 2 == 1))
        lane_p = across_iota((pools, tok))
        pool_id = down_iota((pools, tok))
        lane_s = across_iota((group, tok))
        off = zeros(pools, tok, dtype=I32)
        lo = zeros(group, tok, dtype=I32)
        tab_y = zeros(pools, tok, dtype=I32)
        tab_s = zeros(group, tok, dtype=I32)
        rows_x = []
        for e in range(local):
            target = me * local + e
            hit = fold(jnp.logical_or, [idsbuf[:, layer, k, :] == target for k in range(top)])
            hitb = onehot(hit)
            rank = dot(hitb, before_tok).astype(I32)
            count = jnp.broadcast_to(row_sum(ones(hit)), (group, tok))
            countb = count.astype(BF16)
            count = count.astype(I32)
            amount = dot(pair_of, countb).astype(I32)
            chunks = lax.shift_right_logical(amount + (CHUNK - 1), 4)
            base = dot(before_pool, chunks.astype(F32).astype(BF16)).astype(I32)
            shift = dot(spread, (off * CHUNK).astype(F32).astype(BF16)).astype(I32) + dot(prev, countb).astype(I32)
            keys[e] = jnp.where(hit, rank + shift, -1)
            rows_x.append(jnp.sum(jnp.where((lane_p >= base) & (lane_p < base + chunks), pool_id * pool_chunks + off + lane_p - base, 0).astype(F32),
                                  axis=0, keepdims=True))
            tab_y = jnp.where((lane_p >= off) & (lane_p < off + chunks), e * cap_chunks + base + lane_p - off, tab_y)
            tab_s = jnp.where(lane_s == e, lo, tab_s)
            tab_s = jnp.where(lane_s == local + e, lo + count, tab_s)
            tab_s = jnp.where(lane_s == 2 * local + e, shift - lo, tab_s)
            off = off + chunks
            lo = lo + count
        tabv[0:group, :] = tab_s
        tabv[group:group + pools, :] = jnp.clip(tab_y, 0, local * cap_chunks - 1)
        rows_x.append(zeros(8 - local, tok))
        tabv[tab_x0:tab_x0 + 8, :] = jnp.clip(jnp.concatenate(rows_x, axis=0).astype(I32), 0, pools * pool_chunks - 1)
        tab_copy = pltpu.make_async_copy(tabv, tab, tsem)
        tab_copy.start()
        tab_copy.wait()
        jrow = down_iota((WINDOW, pool_rows))
        diff = across_iota((WINDOW, pool_rows)) - jrow

        def choose(chip, c2):
            halves = []
            for par in BOTH:
                hit = None
                for e in range(local):
                    low_ = tab[2 * chip + par, e]
                    high_ = tab[2 * chip + par, local + e]
                    delta = tab[2 * chip + par, 2 * local + e]
                    this = (diff == delta) & (jrow >= low_) & (jrow < high_)
                    hit = this if hit is None else hit | this
                halves.append(onehot(hit))
            pick[chip] = jnp.concatenate(halves, axis=0)
            return c2

        lax.fori_loop(0, pools, choose, 0, unroll=2)

    own_slots(0)

    def layer_body(layer, carry):
        for b in range(tok // BLOCK):
            for cp in kv_copies(layer, b):
                cp.start()
        for cp in expert_copies(layer):
            cp.start()
        normed = rms_norm(xcur[...].astype(F32))
        for cp in att_copies(layer)[:3]:
            cp.wait()
        kn3[...] = dot(normed, wk[...]).astype(BF16).astype(F32)
        vn3[...] = dot(normed, wv[...]).astype(BF16).astype(F32)
        for h in range(heads):
            if h % 2 == 0:
                pair = dot(normed, wq[:, h * hd:(h + 2) * hd])
            q3[:, h, :] = pair[:, (h % 2) * hd:(h % 2 + 1) * hd].astype(BF16).astype(F32)

        def scores(b, part_):
            kv_copies(layer, b)[0].wait()
            for j in range(BLOCK):
                t = b * BLOCK + j
                q = q3[t]
                s = dot_t(q.astype(BF16), rbuf[pl.ds(t * seq, seq), :]) * scale
                sbuf[part_, j * heads:(j + 1) * heads, :] = jnp.where(lane < len_ref[t], s, -jnp.inf)
                nbuf[part_, j * heads:(j + 1) * heads, :] = q * kn3[pl.ds(t, 1), :]

        def weigh(b, part_):
            s = sbuf[part_]
            sn = row_sum(nbuf[part_]) * scale
            peak = jnp.maximum(row_max(s), sn)
            p = jnp.exp(s - peak)
            pn = jnp.exp(sn - peak)
            inv = 1.0 / (row_sum(p) + pn)
            pb = (p * inv).astype(BF16)
            pnb = (pn * inv).astype(BF16).astype(F32)
            kv_copies(layer, b)[1].wait()
            for j in range(BLOCK):
                t = b * BLOCK + j
                rows = slice(j * heads, (j + 1) * heads)
                o = dot(pb[rows], vbuf[pl.ds(t * seq, seq), :]) + pnb[rows] * vn3[pl.ds(t, 1), :]
                o3[t] = o.astype(BF16).astype(F32)

        def block(i, c2):
            scores(2 * i, 0)
            scores(2 * i + 1, 1)
            weigh(2 * i, 0)
            weigh(2 * i + 1, 1)
            return c2

        def project(w):
            rows = slice(w * span, (w + 1) * span)
            mixed = jnp.concatenate([o3[rows, h, :].astype(BF16) for h in range(heads)], axis=1)
            a = (xcur[rows].astype(F32) + dot(mixed, wo[...])).astype(BF16)
            abuf[rows] = a
            ubuf0[rows] = rms_norm(a.astype(F32))

        started = []

        def go(fn, *args):
            fn(*args).start()
            started.append((fn, args))

        have = set()
        done = set()
        prow = down_iota((pool_rows, tok))

        def gather(dx, dy):
            px, py = at(dx, dy)
            chip = py * nx + px
            for w in range(WAVES):
                across(w, 0, dx, dy).wait_recv()
                across(w, 1, dy, dx).wait_recv()
            halves = []
            for par in BOTH:
                hit = None
                for e in range(local):
                    this = prow == keys[e, pl.ds(2 * chip + par, 1), :]
                    hit = this if hit is None else hit | this
                halves.append(onehot(hit))
            rows = ubuf[pl.ds(2 * chip, 2)].reshape(2 * tok, width)
            xg[pl.ds(chip * pool_chunks, pool_chunks)] = dot(jnp.concatenate(halves, axis=1), rows).astype(BF16).reshape(pool_chunks, CHUNK, width)

        def ready(limit):
            for dy in OFFS:
                for dx in OFFS:
                    if limit and (dx, dy) not in done and all((w, 0, dx, dy) in have and (w, 1, dy, dx) in have for w in range(WAVES)):
                        done.add((dx, dy))
                        gather(dx, dy)
                        limit -= 1

        def s0(w):
            for h in BOTH:
                go(piece, w, h, -1, 0)
                go(piece, w, h, 1, 0)
            for h in BOTH:
                go(piece, w, h, 0, -1)
                go(piece, w, h, 0, 1)
                go(across, w, h, 0, 0)
                have.add((w, h, 0, 0))

        def s2(w):
            for r, p in zip(NEAR, BOTH):
                for h in BOTH:
                    piece(w, h, r, 0).wait_recv()
                    go(piece, w, h, 2, 0, p)
                    go(piece, w, h, r, -1)
                    go(piece, w, h, r, 1)
                    go(across, w, h, r, 0)
                    have.add((w, h, r, 0))

        def s3(w):
            for h in BOTH:
                piece(w, h, 2, 0, 0).wait_recv()
                piece(w, h, 2, 0, 1).wait_recv()
                go(piece, w, h, 2, -1)
                go(piece, w, h, 2, 1)
                go(across, w, h, 2, 0)
                have.add((w, h, 2, 0))

        def s4(w, r):
            for q, p in zip(NEAR, BOTH):
                for h in BOTH:
                    piece(w, h, r, q).wait_recv()
                    go(piece, w, h, r, 2, p)
                    go(across, w, h, r, q)
                    have.add((w, h, r, q))

        def s5(w, r):
            for h in BOTH:
                piece(w, h, r, 2, 0).wait_recv()
                piece(w, h, r, 2, 1).wait_recv()
                go(across, w, h, r, 2)
                have.add((w, h, r, 2))

        blocks = span // (2 * BLOCK)
        lax.fori_loop(0, blocks, block, 0)
        att_copies(layer)[3].wait()
        project(0)
        s0(0)
        lax.fori_loop(blocks, 2 * blocks - 1, block, 0)
        s2(0)
        lax.fori_loop(2 * blocks - 1, 2 * blocks, block, 0)
        s4(0, 0)
        project(1)
        s0(1)
        s3(0)

        att_copies(layer)[4].wait()
        hi, mid, low = split3(wr[...])
        u = ubuf0[...]
        logits = dot(u, hi) + dot(u, mid) + dot(u, low)

        @pl.when(layer + 1 < layers)
        def _():
            for cp in att_copies(layer + 1):
                cp.start()

        e_iota = across_iota((tok, experts))
        hits = [idc[:, k:k + 1] == e_iota for k in range(top)]
        picked = [row_sum(jnp.where(hit, logits, 0.0)) for hit in hits]
        peak = fold(jnp.maximum, picked)
        ex = [jnp.exp(v - peak) for v in picked]
        total = fold(jnp.add, ex)
        columns = [v / total for v in ex] + [slotc[...]]
        columns.append(zeros(tok, LANES - 2 * top))
        gs[...] = jnp.transpose(jnp.concatenate(columns, axis=1))[:2 * top]
        ubuf[me] = u
        for h in BOTH:
            for q in NEXT:
                go(gate_copy, h, q)
        s4(0, -1)
        s4(0, 1)
        s2(1)

        @pl.when(layer == 0)
        def _():
            for d in range(1, group):
                id_copy(d).wait()
            tables(0)

        s4(0, 2)
        s3(1)
        for r in OFFS:
            s5(0, r)
        ready(1)
        s4(1, 0)
        ready(2)

        srow = down_iota((slots, tok))

        def gates(h):
            for q in OFFS:
                if q:
                    gate_copy(h, BACK[q]).wait_recv()
                    table = gsbuf[h, IDX[q]]
                else:
                    table = gs[...]
                slot = table[top:2 * top].astype(I32)
                if h == 0:
                    rel = slot - y * slots
                else:
                    source = lax.shift_right_logical(slot, 6)
                    sx = lax.shift_right_logical(source, 1) & (nx - 1)
                    sy = source // (2 * nx)
                    rel = jnp.where(sx == x, (sy * 2 + (source & 1)) * WINDOW + (slot & (WINDOW - 1)), -1)
                g = zeros(slots, tok)
                for k in range(top):
                    g = jnp.where(srow == rel[k:k + 1], table[k:k + 1], g)
                for i, v in enumerate(split3(jnp.transpose(g))):
                    gmat[h * 4 + IDX[q], i * tok:(i + 1) * tok, :] = v

        s4(1, -1)
        s4(1, 1)
        ready(2)
        s4(1, 2)
        ready(3)
        s5(1, 0)
        ready(2)
        s5(1, -1)
        s5(1, 1)
        ready(4)
        s5(1, 2)
        ready(pools)

        for cp in expert_copies(layer):
            cp.wait()

        def tile(i, c2):
            e = i // per_expert
            first_chunk = (i % per_expert) * per
            for j in range(per):
                xt[j * CHUNK:(j + 1) * CHUNK, :] = xg[tab[tab_x0 + e, first_chunk + j]]
            rows_in = xt[...]
            first = dot(rows_in, wg[e])
            second = dot(rows_in, wu[e])
            act[i] = (first * sigmoid(first) * second).astype(BF16)
            return c2

        lax.fori_loop(0, local * per_expert, tile, 0)
        for fn, args in started:
            fn(*args).wait_send()
        started.clear()

        firsts = [(2, 0), (2, 1), (1, 0), (-1, 0), (1, 1), (-1, 1), (0, 1)]
        head = [max(w - w % 2, min(w, 1)) for w in range(steps)]
        for w in range(steps):
            lead = head[w]
            count_ = head.count(lead)
            if w == lead:
                def down(i, c2):
                    out = dot(act[i], wd[i // per_expert, :, w * 2 * LANES:(w + count_) * 2 * LANES])
                    yq[pl.ds(i * per, per), :, :count_ * 2 * LANES] = out.astype(BF16).reshape(per, CHUNK, count_ * 2 * LANES)
                    return c2

                lax.fori_loop(0, local * per_expert, down, 0, unroll=2)

            def window(chip, c2):
                inside = slice((w - lead) * 2 * LANES, (w - lead + 1) * 2 * LANES)
                rows = jnp.concatenate([yq[tab[tab_y0 + chip, i], :, inside] for i in range(pool_chunks)], axis=0)
                out = dot(pick[chip], rows).astype(BF16)
                cy = chip // nx
                cx = chip % nx
                for h in BOTH:
                    one, two = axes(h, cx, cy)
                    for par in BOTH:
                        row = pl.multiple_of(window_row(h * steps + w, one, par, two), WINDOW)
                        rbuf[pl.ds(row, WINDOW), :] = out[par * WINDOW:(par + 1) * WINDOW, h * LANES:(h + 1) * LANES]
                return c2

            lax.fori_loop(0, pools, window, 0, unroll=4)
            for r, flip in firsts:
                for h in BOTH:
                    go(first_copy, h, w, r, flip)
            for h in BOTH:
                size = ny * WINDOW
                own = pl.ds(pl.multiple_of(window_row(h * steps + w, (x, y)[h], core), size), size)
                vbuf[own, :] = rbuf[own, :]

        def merge(h, ws):
            for w in ws:
                for r, flip in firsts:
                    first_copy(h, w, r, flip).wait_recv()
            for q in (2, 1, -1, 0):
                two = at(q, q)[1 - h]
                rows = []
                for s in range(2 * nx):
                    pieces = [vbuf[pl.ds(pl.multiple_of(window_row(h * steps + w, s // 2, s % 2, two), WINDOW), WINDOW), :] for w in ws]
                    rows.append(jnp.concatenate(pieces, axis=1))
                parts = dot(gmat[h * 4 + IDX[q]], jnp.concatenate(rows, axis=0))
                total = parts[0:tok] + parts[tok:2 * tok] + parts[2 * tok:3 * tok]
                for i, w in enumerate(ws):
                    part[h * steps + w, IDX[q]] = total[:, i * LANES:(i + 1) * LANES]
                if q:
                    for w in ws:
                        go(second_copy, h, w, q)

        for h in BOTH:
            gates(h)
        for h in BOTH:
            merge(h, (0, 1))

        @pl.when(layer + 1 < layers)
        def _():
            own_slots(layer + 1)
            tables(layer + 1)

        for w in range(2, steps):
            for h in BOTH:
                merge(h, (w,))
        for w in range(steps):
            for h in BOTH:
                n = h * steps + w
                where = slice((w * 2 + h) * LANES, (w * 2 + h + 1) * LANES)
                for q in NEXT:
                    second_copy(h, w, q).wait_recv()
                total = (part[n, 0] + final[n, 1]) + (final[n, 2] + final[n, 3])
                xcur[:, where] = (abuf[:, where].astype(F32) + total).astype(BF16)
        for fn, args in started:
            fn(*args).wait_send()
        return carry

    lax.fori_loop(0, layers, layer_body, 0)
    x_ref[...] = xcur[...]


def solution(mesh):
    ny, nx = mesh.shape['pool'], mesh.shape['ep'] // 2

    def device_step(hidden, k_cache, v_cache, lengths, w_query, w_key, w_value, w_out, w_router, expert_ids, w_gate, w_up, w_down):
        tok, width = hidden.shape
        layers, _, top = expert_ids.shape
        seq, hd = k_cache.shape[2], k_cache.shape[4]
        heads = w_query.shape[2] // hd
        experts = w_router.shape[2]
        local, ff = w_gate.shape[1], w_gate.shape[3]
        pools = nx * ny
        group = 2 * pools
        k_cache = k_cache.reshape(layers, tok * seq, hd)
        v_cache = v_cache.reshape(layers, tok * seq, hd)
        mine = jnp.swapaxes(expert_ids, 1, 2)
        pool_chunks = (2 * (WINDOW - 1) + local * (CHUNK - 1)) // CHUNK
        most = 2 * group * tok * top // (group * local)
        per = TILE // CHUNK
        cap_chunks = pl.cdiv((most + pools * (CHUNK - 1)) // CHUNK, per) * per
        steps = width // (2 * LANES)
        vm = pl.BlockSpec(memory_space=pltpu.VMEM)
        hb = pl.BlockSpec(memory_space=pl.ANY)
        sm = pl.BlockSpec(memory_space=pltpu.SMEM)
        dma = pltpu.SemaphoreType.DMA
        dims = (ny, nx, layers, tok, width, heads, hd, seq, experts, local, top, pool_chunks, cap_chunks)
        return pl.pallas_call(
            functools.partial(step_kernel, dims),
            out_shape=jax.ShapeDtypeStruct((tok, width), BF16),
            in_specs=[vm, hb, hb, sm, hb, hb, hb, hb, hb, vm, hb, hb, hb],
            out_specs=vm,
            scratch_shapes=[
                vmem(tok, width), vmem(tok, width), vmem(tok, width), pltpu.VMEM((2 * top, tok), F32),
                pltpu.VMEM((tok, LANES), I32), pltpu.VMEM((tok, top), F32),
                pltpu.VMEM((tok, heads, hd), F32), pltpu.VMEM((tok, heads, hd), F32),
                pltpu.VMEM((2, BLOCK * heads, seq), F32), pltpu.VMEM((2, BLOCK * heads, hd), F32), pltpu.VMEM((tok, hd), F32), pltpu.VMEM((tok, hd), F32),
                vmem(width, heads * hd), vmem(width, hd), vmem(width, hd),
                vmem(heads * hd, width), pltpu.VMEM((width, experts), F32),
                pltpu.VMEM((group,) + mine.shape, I32), pltpu.VMEM((local, group, tok), I32),
                pltpu.VMEM((group + pools + 8, tok), I32), pltpu.SMEM((group + pools + 8, tok), I32),
                vmem(group, tok, width),
                vmem(pools * pool_chunks, CHUNK, width), vmem(TILE, width),
                vmem(local * cap_chunks // per, TILE, ff), vmem(local * cap_chunks, CHUNK, 4 * LANES),
                vmem(pools, 2 * WINDOW, pool_chunks * CHUNK),
                vmem(tok * seq, LANES), vmem(tok * seq, LANES),
                vmem(8, 3 * tok, 2 * nx * WINDOW),
                pltpu.VMEM((2 * steps, 4, tok, LANES), F32), pltpu.VMEM((2 * steps, 4, tok, LANES), F32), pltpu.VMEM((2, 4, 2 * top, tok), F32),
                vmem(local, width, ff), vmem(local, width, ff), vmem(local, ff, width),
                dma((tok // BLOCK,)), dma((tok // BLOCK,)), dma((5,)), dma((3, local)), dma,
                dma((group,)), dma((group,)), dma((128,)), dma((128,)), dma((64,)), dma((64,)), dma((8,)), dma((8,)),
                dma((16 * steps,)), dma((16 * steps,)), dma((8 * steps,)), dma((8 * steps,)),
            ],
            compiler_params=pltpu.CompilerParams(vmem_limit_bytes=67043328, collective_id=0, has_side_effects=True),
            name='step',
        )(hidden, k_cache, v_cache, lengths, w_query, w_key, w_value, w_out, w_router, mine, w_gate, w_up, w_down)

    cache_spec = P(None, BATCH_AXES, None, None, None)
    expert_spec = P(None, GROUP_AXES, None, None)
    in_specs = (P(BATCH_AXES, None), cache_spec, cache_spec, P(BATCH_AXES), P(), P(), P(), P(), P(), P(None, BATCH_AXES, None), expert_spec, expert_spec, expert_spec)
    return jax.shard_map(device_step, mesh=mesh, in_specs=in_specs, out_specs=P(BATCH_AXES, None), check_vma=False)
```

```python
import functools

import jax
import jax.numpy as jnp
from jax import lax
from jax.experimental import pallas as pl
from jax.experimental.pallas import tpu as pltpu
from jax.sharding import PartitionSpec as P

EPS = 1e-6
GROUP_AXES = ('pool', 'ep')
BATCH_AXES = ('dp', 'pool', 'ep')
F32 = jnp.float32
BF16 = jnp.bfloat16
I32 = jnp.int32
CHUNK = 16
WINDOW = 64
TILE = 768
LANES = 128
BLOCK = 16
WAVES = 2
MESH = pl.DeviceIdType.MESH
OFFS = (0, -1, 1, 2)
IDX = {0: 0, 1: 1, -1: 2, 2: 3}
BACK = {1: -1, -1: 1, 2: 2}
NEAR = OFFS[1:3]
NEXT = OFFS[1:]
FAR = OFFS[-1]
BOTH = range(2)
ROWS, COLS = BOTH


def rms_norm(wide):
    return (wide * lax.rsqrt(jnp.mean(wide * wide, axis=-1, keepdims=True) + EPS)).astype(BF16)


def dot(a, b):
    return jnp.dot(a, b, preferred_element_type=F32)


def dot_t(a, b):
    return lax.dot_general(a, b, (((1,), (1,)), ((), ())), preferred_element_type=F32)


def split3(w):
    hi = w.astype(BF16)
    rest = w - hi.astype(F32)
    mid = rest.astype(BF16)
    low = (rest - mid.astype(F32)).astype(BF16)
    return hi, mid, low


def iota(shape, axis):
    return lax.broadcasted_iota(I32, shape, axis)


def ones(cond):
    return jnp.where(cond, 1.0, 0.0)


def onehot(cond):
    return ones(cond).astype(BF16)


def zeros(*shape, dtype=F32):
    return jnp.zeros(shape, dtype)


def row_max(v):
    return jnp.max(v, axis=1, keepdims=True)


def row_sum(v):
    return jnp.sum(v, axis=1, keepdims=True)


def sigmoid(v):
    return 1.0 / (1.0 + jnp.exp(-v))


def down_iota(shape):
    return iota(shape, 0)


def across_iota(shape):
    return iota(shape, 1)


def fold(fn, values):
    return functools.reduce(fn, values)


def vmem(*shape, dtype=BF16):
    return pltpu.VMEM(shape, dtype)


def step_kernel(dims, hidden_ref, kc_hbm, vc_hbm, len_ref, wq_hbm, wk_hbm, wv_hbm, wo_hbm, wr_hbm, mine_ref, wg_hbm, wu_hbm, wd_hbm,
                x_ref,
                xcur, abuf, ubuf0, gs, idc, slotc, q3, o3, sbuf, nbuf, kn3, vn3, wq, wk, wv, wo, wr,
                idsbuf, keys, tabv, tab, ubuf, xg, xt, act, yq, pick, rbuf, vbuf, gmat, part, final, gsbuf, wg, wu, wd,
                ksem, vsem, asem, wsem, tsem, id_send, id_recv, ag_send, ag_recv, dd_send, dd_recv, gs_send, gs_recv,
                p1_send, p1_recv, p2_send, p2_recv):
    ny, nx, layers, tok, width, heads, hd, seq, experts, local, top, pool_chunks, cap_chunks = dims
    pools = ny * nx
    group = 2 * pools
    pair_lanes = 2 * LANES
    pool_rows = pool_chunks * CHUNK
    span = tok // WAVES
    half = span // 2
    steps = width // (2 * LANES)
    per = TILE // CHUNK
    per_expert = cap_chunks // per
    slots = 2 * nx * WINDOW
    y = lax.axis_index('pool')
    ep = lax.axis_index('ep')
    x = ep // 2
    core = lax.rem(ep, 2)
    other = 1 - core
    me = y * (2 * nx) + ep

    def at(dx, dy):
        return lax.rem(x + dx + nx, nx), lax.rem(y + dy + ny, ny)

    def dev(dx, dy, c):
        px, py = at(dx, dy)
        return {'pool': py, 'ep': px * 2 + c}

    def number(dx, dy, c):
        px, py = at(dx, dy)
        return py * (2 * nx) + px * 2 + c

    def axes(h, first, second):
        return (first, second) if h == 0 else (second, first)

    def peer(d):
        to = lax.rem(me + d, group)
        return {'pool': to // (2 * nx), 'ep': lax.rem(to, 2 * nx)}

    def remote(src, dst, send, recv, device):
        return pltpu.make_async_remote_copy(src_ref=src, dst_ref=dst, send_sem=send, recv_sem=recv, device_id=device, device_id_type=MESH)

    def att_copies(layer):
        return [pltpu.make_async_copy(src.at[layer], dst, asem.at[i])
                for i, (src, dst) in enumerate(((wq_hbm, wq), (wk_hbm, wk), (wv_hbm, wv), (wo_hbm, wo), (wr_hbm, wr)))]

    def expert_copies(layer):
        return [pltpu.make_async_copy(src.at[layer, e], dst.at[e], wsem.at[i, e])
                for i, (src, dst) in enumerate(((wg_hbm, wg), (wu_hbm, wu), (wd_hbm, wd))) for e in range(local)]

    def kv_copies(layer, b):
        rows = pl.ds(b * (BLOCK * seq), BLOCK * seq)
        return (pltpu.make_async_copy(kc_hbm.at[layer, rows], rbuf.at[rows], ksem.at[b]),
                pltpu.make_async_copy(vc_hbm.at[layer, rows], vbuf.at[rows], vsem.at[b]))

    def id_copy(d):
        return remote(mine_ref, idsbuf.at[me], id_send.at[d], id_recv.at[d], peer(d))

    def piece(w, h, r, q, p=None):
        if q == 0:
            step = 1 if (r == -1 or (r == 2 and p == 0)) else -1
            own = (0, 0) if r in (1, -1) else (-step, 0)
            to = (step, 0)
        else:
            step = 1 if (q == -1 or (q == 2 and p == 0)) else -1
            own = (r, 0) if q in (1, -1) else (r, -step)
            to = (0, step)
        first = w * span + h * half
        rows = pl.ds(first, half) if p is None else pl.ds(first + p * (half // 2), half // 2)
        owner = number(*axes(h, *own), core)
        src = ubuf0.at[rows] if own == (0, 0) else ubuf.at[owner, rows]
        sem = (((w * 2 + h) * 4 + IDX[r]) * 4 + IDX[q]) * 2 + (p or 0)
        return remote(src, ubuf.at[owner, rows], ag_send.at[sem], ag_recv.at[sem], dev(*axes(h, *to), core))

    def across(w, h, r, q):
        rows = pl.ds(w * span + h * half, half)
        owner = number(*axes(h, r, q), core)
        src = ubuf0.at[rows] if (r, q) == (0, 0) else ubuf.at[owner, rows]
        sem = ((w * 2 + h) * 4 + IDX[r]) * 4 + IDX[q]
        return remote(src, ubuf.at[owner, rows], dd_send.at[sem], dd_recv.at[sem], dev(0, 0, other))

    def gate_copy(h, q):
        back = IDX[BACK[q]]
        sem = h * 4 + back
        return remote(gs, gsbuf.at[h, back], gs_send.at[sem], gs_recv.at[sem], dev(*axes(h, 0, q), core))

    def window_row(n, one, c, two=0):
        return ((n * nx + one) * 2 + c) * (ny * WINDOW) + two * WINDOW

    def first_copy(h, w, r, flip):
        n = h * steps + w
        c = other if flip else core
        size = ny * WINDOW
        src = pl.ds(pl.multiple_of(window_row(n, at(r, r)[h], c), size), size)
        dst = pl.ds(pl.multiple_of(window_row(n, (x, y)[h], core), size), size)
        sem = (n * 4 + IDX[r]) * 2 + flip
        return remote(rbuf.at[src], vbuf.at[dst], p1_send.at[sem], p1_recv.at[sem], dev(*axes(h, r, 0), c))

    def second_copy(h, w, q):
        n = h * steps + w
        sem = n * 4 + IDX[q]
        return remote(part.at[n, IDX[q]], final.at[n, IDX[q]], p2_send.at[sem], p2_recv.at[sem], dev(*axes(h, 0, q), core))

    for cp in att_copies(0):
        cp.start()
    barrier = pltpu.get_barrier_semaphore()
    for d in range(1, group):
        pl.semaphore_signal(barrier, inc=1, device_id=peer(d), device_id_type=MESH)
    pl.semaphore_wait(barrier, group - 1)
    for d in range(1, group):
        id_copy(d).start()
    idsbuf[me] = mine_ref[...]
    xcur[...] = hidden_ref[...]
    scale = hd ** -0.5
    lane = across_iota((heads, seq))

    tab_y0 = group
    tab_x0 = group + pools

    def own_slots(layer):
        e_iota = across_iota((tok, experts))
        before = onehot(across_iota((tok, tok)) < down_iota((tok, tok)))
        e_row = down_iota((experts, experts))
        e_col = across_iota((experts, experts))
        same = onehot((e_row < e_col) & (e_row // local == e_col // local))
        ids = jnp.concatenate([mine_ref[layer].astype(F32), zeros(LANES - top, tok)], axis=0)
        ids = jnp.transpose(ids).astype(I32)
        idc[...] = ids
        hits = [ids[:, k:k + 1] == e_iota for k in range(top)]
        chosen = fold(jnp.logical_or, hits)
        chosen = ones(chosen)
        rank = dot(before, chosen.astype(BF16))
        count = jnp.sum(chosen, axis=0, keepdims=True)
        start = dot(jnp.broadcast_to(count, (8, experts)).astype(BF16), same)[0:1]
        slot_full = rank + start + ((e_iota // local) * WINDOW).astype(F32)
        for k in range(top):
            slotc[:, k:k + 1] = row_sum(jnp.where(hits[k], slot_full, 0.0))

    def tables(layer):
        before_tok = onehot(down_iota((tok, tok)) < across_iota((tok, tok)))
        before_pool = onehot(across_iota((pools, pools)) < down_iota((pools, pools)))
        pair_of = onehot(across_iota((pools, group)) // 2 == down_iota((pools, group)))
        spread = onehot(down_iota((group, pools)) // 2 == across_iota((group, pools)))
        prev = onehot((across_iota((group, group)) + 1 == down_iota((group, group))) & (down_iota((group, group)) % 2 == 1))
        lane_p = across_iota((pools, tok))
        pool_id = down_iota((pools, tok))
        lane_s = across_iota((group, tok))
        off = zeros(pools, tok, dtype=I32)
        lo = zeros(group, tok, dtype=I32)
        tab_y = zeros(pools, tok, dtype=I32)
        tab_s = zeros(group, tok, dtype=I32)
        rows_x = []
        for e in range(local):
            target = me * local + e
            hit = fold(jnp.logical_or, [idsbuf[:, layer, k, :] == target for k in range(top)])
            hitb = onehot(hit)
            rank = dot(hitb, before_tok).astype(I32)
            count = jnp.broadcast_to(row_sum(ones(hit)), (group, tok))
            countb = count.astype(BF16)
            count = count.astype(I32)
            amount = dot(pair_of, countb).astype(I32)
            chunks = lax.shift_right_logical(amount + (CHUNK - 1), 4)
            base = dot(before_pool, chunks.astype(F32).astype(BF16)).astype(I32)
            shift = dot(spread, (off * CHUNK).astype(F32).astype(BF16)).astype(I32) + dot(prev, countb).astype(I32)
            keys[e] = jnp.where(hit, rank + shift, -1)
            rows_x.append(jnp.sum(jnp.where((lane_p >= base) & (lane_p < base + chunks), pool_id * pool_chunks + off + lane_p - base, 0).astype(F32),
                                  axis=0, keepdims=True))
            tab_y = jnp.where((lane_p >= off) & (lane_p < off + chunks), e * cap_chunks + base + lane_p - off, tab_y)
            tab_s = jnp.where(lane_s == e, lo, tab_s)
            tab_s = jnp.where(lane_s == local + e, lo + count, tab_s)
            tab_s = jnp.where(lane_s == 2 * local + e, shift - lo, tab_s)
            off = off + chunks
            lo = lo + count
        tabv[0:group, :] = tab_s
        tabv[group:group + pools, :] = jnp.clip(tab_y, 0, local * cap_chunks - 1)
        rows_x.append(zeros(8 - local, tok))
        tabv[tab_x0:tab_x0 + 8, :] = jnp.clip(jnp.concatenate(rows_x, axis=0).astype(I32), 0, pools * pool_chunks - 1)
        tab_copy = pltpu.make_async_copy(tabv, tab, tsem)
        tab_copy.start()
        tab_copy.wait()
        jrow = down_iota((WINDOW, pool_rows))
        diff = across_iota((WINDOW, pool_rows)) - jrow

        def choose(chip, c2):
            halves = []
            for par in BOTH:
                hit = None
                for e in range(local):
                    low_ = tab[2 * chip + par, e]
                    high_ = tab[2 * chip + par, local + e]
                    delta = tab[2 * chip + par, 2 * local + e]
                    this = (diff == delta) & (jrow >= low_) & (jrow < high_)
                    hit = this if hit is None else hit | this
                halves.append(onehot(hit))
            pick[chip] = jnp.concatenate(halves, axis=0)
            return c2

        lax.fori_loop(0, pools, choose, 0, unroll=2)

    own_slots(0)

    def layer_body(layer, carry):
        for b in range(tok // BLOCK):
            for cp in kv_copies(layer, b):
                cp.start()
        for cp in expert_copies(layer):
            cp.start()
        normed = rms_norm(xcur[...].astype(F32))
        for cp in att_copies(layer)[:3]:
            cp.wait()
        kn3[...] = dot(normed, wk[...]).astype(BF16).astype(F32)
        vn3[...] = dot(normed, wv[...]).astype(BF16).astype(F32)
        for h in range(heads):
            if h % 2 == 0:
                pair = dot(normed, wq[:, h * hd:(h + 2) * hd])
            q3[:, h, :] = pair[:, (h % 2) * hd:(h % 2 + 1) * hd].astype(BF16).astype(F32)

        def scores(b, part_):
            kv_copies(layer, b)[0].wait()
            for j in range(BLOCK):
                t = b * BLOCK + j
                q = q3[t]
                s = dot_t(q.astype(BF16), rbuf[pl.ds(t * seq, seq), :]) * scale
                sbuf[part_, j * heads:(j + 1) * heads, :] = jnp.where(lane < len_ref[t], s, -jnp.inf)
                nbuf[part_, j * heads:(j + 1) * heads, :] = q * kn3[pl.ds(t, 1), :]

        def weigh(b, part_):
            s = sbuf[part_]
            sn = row_sum(nbuf[part_]) * scale
            peak = jnp.maximum(row_max(s), sn)
            p = jnp.exp(s - peak)
            pn = jnp.exp(sn - peak)
            inv = 1.0 / (row_sum(p) + pn)
            pb = (p * inv).astype(BF16)
            pnb = (pn * inv).astype(BF16).astype(F32)
            kv_copies(layer, b)[1].wait()
            for j in range(BLOCK):
                t = b * BLOCK + j
                rows = slice(j * heads, (j + 1) * heads)
                o = dot(pb[rows], vbuf[pl.ds(t * seq, seq), :]) + pnb[rows] * vn3[pl.ds(t, 1), :]
                o3[t] = o.astype(BF16).astype(F32)

        def block(i, c2):
            scores(2 * i, 0)
            scores(2 * i + 1, 1)
            weigh(2 * i, 0)
            weigh(2 * i + 1, 1)
            return c2

        def project(w):
            rows = slice(w * span, (w + 1) * span)
            mixed = jnp.concatenate([o3[rows, h, :].astype(BF16) for h in range(heads)], axis=1)
            a = (xcur[rows].astype(F32) + dot(mixed, wo[...])).astype(BF16)
            abuf[rows] = a
            ubuf0[rows] = rms_norm(a.astype(F32))

        started = []

        def go(fn, *args):
            fn(*args).start()
            started.append((fn, args))

        have = set()
        done = set()
        prow = down_iota((pool_rows, tok))

        def gather(dx, dy):
            px, py = at(dx, dy)
            chip = py * nx + px
            for w in range(WAVES):
                across(w, 0, dx, dy).wait_recv()
                across(w, 1, dy, dx).wait_recv()
            halves = []
            for par in BOTH:
                hit = None
                for e in range(local):
                    this = prow == keys[e, pl.ds(2 * chip + par, 1), :]
                    hit = this if hit is None else hit | this
                halves.append(onehot(hit))
            rows = ubuf[pl.ds(2 * chip, 2)].reshape(2 * tok, width)
            xg[pl.ds(chip * pool_chunks, pool_chunks)] = dot(jnp.concatenate(halves, axis=1), rows).astype(BF16).reshape(pool_chunks, CHUNK, width)

        def ready(limit):
            for dy in OFFS:
                for dx in OFFS:
                    if limit and (dx, dy) not in done and all((w, 0, dx, dy) in have and (w, 1, dy, dx) in have for w in range(WAVES)):
                        done.add((dx, dy))
                        gather(dx, dy)
                        limit -= 1

        def s0(w):
            for h in BOTH:
                go(piece, w, h, -1, 0)
                go(piece, w, h, 1, 0)
            for h in BOTH:
                go(piece, w, h, 0, -1)
                go(piece, w, h, 0, 1)
                go(across, w, h, 0, 0)
                have.add((w, h, 0, 0))

        def s2(w):
            for r, p in zip(NEAR, BOTH):
                for h in BOTH:
                    piece(w, h, r, 0).wait_recv()
                    go(piece, w, h, 2, 0, p)
                    go(piece, w, h, r, -1)
                    go(piece, w, h, r, 1)
                    go(across, w, h, r, 0)
                    have.add((w, h, r, 0))

        def s3(w):
            for h in BOTH:
                piece(w, h, 2, 0, 0).wait_recv()
                piece(w, h, 2, 0, 1).wait_recv()
                go(piece, w, h, 2, -1)
                go(piece, w, h, 2, 1)
                go(across, w, h, 2, 0)
                have.add((w, h, 2, 0))

        def s4(w, r):
            for q, p in zip(NEAR, BOTH):
                for h in BOTH:
                    piece(w, h, r, q).wait_recv()
                    go(piece, w, h, r, 2, p)
                    go(across, w, h, r, q)
                    have.add((w, h, r, q))

        def s5(w, r):
            for h in BOTH:
                piece(w, h, r, 2, 0).wait_recv()
                piece(w, h, r, 2, 1).wait_recv()
                go(across, w, h, r, 2)
                have.add((w, h, r, 2))

        blocks = span // (2 * BLOCK)
        lax.fori_loop(0, blocks, block, 0)
        att_copies(layer)[3].wait()
        project(0)
        s0(0)
        lax.fori_loop(blocks, 2 * blocks - 1, block, 0)
        lax.fori_loop(2 * blocks - 1, 2 * blocks, block, 0)
        s2(0)
        project(1)
        s0(1)
        s4(0, 0)
        s3(0)

        att_copies(layer)[4].wait()
        hi, mid, low = split3(wr[...])
        u = ubuf0[...]
        logits = dot(u, hi) + dot(u, mid) + dot(u, low)

        @pl.when(layer + 1 < layers)
        def _():
            for cp in att_copies(layer + 1):
                cp.start()

        e_iota = across_iota((tok, experts))
        hits = [idc[:, k:k + 1] == e_iota for k in range(top)]
        picked = [row_sum(jnp.where(hit, logits, 0.0)) for hit in hits]
        peak = fold(jnp.maximum, picked)
        ex = [jnp.exp(v - peak) for v in picked]
        total = fold(jnp.add, ex)
        columns = [v / total for v in ex] + [slotc[...]]
        columns.append(zeros(tok, LANES - 2 * top))
        gs[...] = jnp.transpose(jnp.concatenate(columns, axis=1))[:2 * top]
        ubuf[me] = u
        for h in BOTH:
            for q in NEXT:
                go(gate_copy, h, q)
        s4(0, -1)
        s4(0, 1)
        s2(1)

        @pl.when(layer == 0)
        def _():
            for d in range(1, group):
                id_copy(d).wait()
            tables(0)

        s4(0, 2)
        s3(1)
        for r in OFFS:
            s5(0, r)
        ready(1)
        s4(1, 0)
        ready(2)

        srow = down_iota((slots, tok))

        def gates(h):
            for q in OFFS:
                if q:
                    gate_copy(h, BACK[q]).wait_recv()
                    table = gsbuf[h, IDX[q]]
                else:
                    table = gs[...]
                slot = table[top:2 * top].astype(I32)
                if h == 0:
                    rel = slot - y * slots
                else:
                    source = lax.shift_right_logical(slot, 6)
                    sx = lax.shift_right_logical(source, 1) & (nx - 1)
                    sy = source // (2 * nx)
                    rel = jnp.where(sx == x, (sy * 2 + (source & 1)) * WINDOW + (slot & (WINDOW - 1)), -1)
                g = zeros(slots, tok)
                for k in range(top):
                    g = jnp.where(srow == rel[k:k + 1], table[k:k + 1], g)
                for i, v in enumerate(split3(jnp.transpose(g))):
                    gmat[h * 4 + IDX[q], i * tok:(i + 1) * tok, :] = v

        s4(1, -1)
        s4(1, 1)
        ready(2)
        s4(1, 2)
        ready(3)
        s5(1, 0)
        ready(2)
        s5(1, -1)
        s5(1, 1)
        ready(4)
        s5(1, 2)
        ready(pools)

        for cp in expert_copies(layer):
            cp.wait()

        def tile(i, c2):
            e = i // per_expert
            first_chunk = (i % per_expert) * per
            for j in range(per):
                xt[j * CHUNK:(j + 1) * CHUNK, :] = xg[tab[tab_x0 + e, first_chunk + j]]
            rows_in = xt[...]
            first = dot(rows_in, wg[e])
            second = dot(rows_in, wu[e])
            act[i] = (first * sigmoid(first) * second).astype(BF16)
            return c2

        lax.fori_loop(0, local * per_expert, tile, 0)
        for fn, args in started:
            fn(*args).wait_send()
        started.clear()

        firsts = [(2, 0), (2, 1), (1, 0), (-1, 0), (1, 1), (-1, 1), (0, 1)]
        head = [max(w - w % 2, min(w, 1)) for w in range(steps)]
        for w in range(steps):
            lead = head[w]
            count_ = head.count(lead)
            if w == lead:
                def down(i, c2):
                    out = dot(act[i], wd[i // per_expert, :, w * 2 * LANES:(w + count_) * 2 * LANES])
                    yq[pl.ds(i * per, per), :, :count_ * 2 * LANES] = out.astype(BF16).reshape(per, CHUNK, count_ * 2 * LANES)
                    return c2

                lax.fori_loop(0, local * per_expert, down, 0, unroll=2)

            def window(chip, c2):
                inside = slice((w - lead) * 2 * LANES, (w - lead + 1) * 2 * LANES)
                rows = jnp.concatenate([yq[tab[tab_y0 + chip, i], :, inside] for i in range(pool_chunks)], axis=0)
                out = dot(pick[chip], rows).astype(BF16)
                cy = chip // nx
                cx = chip % nx
                for h in BOTH:
                    one, two = axes(h, cx, cy)
                    for par in BOTH:
                        row = pl.multiple_of(window_row(h * steps + w, one, par, two), WINDOW)
                        rbuf[pl.ds(row, WINDOW), :] = out[par * WINDOW:(par + 1) * WINDOW, h * LANES:(h + 1) * LANES]
                return c2

            lax.fori_loop(0, pools, window, 0, unroll=8)
            for r, flip in firsts:
                for h in BOTH:
                    go(first_copy, h, w, r, flip)
            for h in BOTH:
                size = ny * WINDOW
                own = pl.ds(pl.multiple_of(window_row(h * steps + w, (x, y)[h], core), size), size)
                vbuf[own, :] = rbuf[own, :]

        def merge(h, ws):
            for w in ws:
                for r, flip in firsts:
                    first_copy(h, w, r, flip).wait_recv()
            for q in (2, 1, -1, 0):
                two = at(q, q)[1 - h]
                rows = []
                for s in range(2 * nx):
                    pieces = [vbuf[pl.ds(pl.multiple_of(window_row(h * steps + w, s // 2, s % 2, two), WINDOW), WINDOW), :] for w in ws]
                    rows.append(jnp.concatenate(pieces, axis=1))
                parts = dot(gmat[h * 4 + IDX[q]], jnp.concatenate(rows, axis=0))
                total = parts[0:tok] + parts[tok:2 * tok] + parts[2 * tok:3 * tok]
                for i, w in enumerate(ws):
                    part[h * steps + w, IDX[q]] = total[:, i * LANES:(i + 1) * LANES]
                if q:
                    for w in ws:
                        go(second_copy, h, w, q)

        for h in BOTH:
            gates(h)
        for h in BOTH:
            merge(h, (0, 1))

        @pl.when(layer + 1 < layers)
        def _():
            own_slots(layer + 1)
            tables(layer + 1)

        for w in range(2, steps):
            for h in BOTH:
                merge(h, (w,))
        for w in range(steps):
            for h in BOTH:
                n = h * steps + w
                where = slice((w * 2 + h) * LANES, (w * 2 + h + 1) * LANES)
                for q in NEXT:
                    second_copy(h, w, q).wait_recv()
                total = (part[n, 0] + final[n, 1]) + (final[n, 2] + final[n, 3])
                xcur[:, where] = (abuf[:, where].astype(F32) + total).astype(BF16)
        for fn, args in started:
            fn(*args).wait_send()
        return carry

    lax.fori_loop(0, layers, layer_body, 0)
    x_ref[...] = xcur[...]


def solution(mesh):
    ny, nx = mesh.shape['pool'], mesh.shape['ep'] // 2

    def device_step(hidden, k_cache, v_cache, lengths, w_query, w_key, w_value, w_out, w_router, expert_ids, w_gate, w_up, w_down):
        tok, width = hidden.shape
        layers, _, top = expert_ids.shape
        seq, hd = k_cache.shape[2], k_cache.shape[4]
        heads = w_query.shape[2] // hd
        experts = w_router.shape[2]
        local, ff = w_gate.shape[1], w_gate.shape[3]
        pools = nx * ny
        group = 2 * pools
        k_cache = k_cache.reshape(layers, tok * seq, hd)
        v_cache = v_cache.reshape(layers, tok * seq, hd)
        mine = jnp.swapaxes(expert_ids, 1, 2)
        pool_chunks = (2 * (WINDOW - 1) + local * (CHUNK - 1)) // CHUNK
        most = 2 * group * tok * top // (group * local)
        per = TILE // CHUNK
        cap_chunks = pl.cdiv((most + pools * (CHUNK - 1)) // CHUNK, per) * per
        steps = width // (2 * LANES)
        vm = pl.BlockSpec(memory_space=pltpu.VMEM)
        hb = pl.BlockSpec(memory_space=pl.ANY)
        sm = pl.BlockSpec(memory_space=pltpu.SMEM)
        dma = pltpu.SemaphoreType.DMA
        dims = (ny, nx, layers, tok, width, heads, hd, seq, experts, local, top, pool_chunks, cap_chunks)
        return pl.pallas_call(
            functools.partial(step_kernel, dims),
            out_shape=jax.ShapeDtypeStruct((tok, width), BF16),
            in_specs=[vm, hb, hb, sm, hb, hb, hb, hb, hb, vm, hb, hb, hb],
            out_specs=vm,
            scratch_shapes=[
                vmem(tok, width), vmem(tok, width), vmem(tok, width), pltpu.VMEM((2 * top, tok), F32),
                pltpu.VMEM((tok, LANES), I32), pltpu.VMEM((tok, top), F32),
                pltpu.VMEM((tok, heads, hd), F32), pltpu.VMEM((tok, heads, hd), F32),
                pltpu.VMEM((2, BLOCK * heads, seq), F32), pltpu.VMEM((2, BLOCK * heads, hd), F32), pltpu.VMEM((tok, hd), F32), pltpu.VMEM((tok, hd), F32),
                vmem(width, heads * hd), vmem(width, hd), vmem(width, hd),
                vmem(heads * hd, width), pltpu.VMEM((width, experts), F32),
                pltpu.VMEM((group,) + mine.shape, I32), pltpu.VMEM((local, group, tok), I32),
                pltpu.VMEM((group + pools + 8, tok), I32), pltpu.SMEM((group + pools + 8, tok), I32),
                vmem(group, tok, width),
                vmem(pools * pool_chunks, CHUNK, width), vmem(TILE, width),
                vmem(local * cap_chunks // per, TILE, ff), vmem(local * cap_chunks, CHUNK, 4 * LANES),
                vmem(pools, 2 * WINDOW, pool_chunks * CHUNK),
                vmem(tok * seq, LANES), vmem(tok * seq, LANES),
                vmem(8, 3 * tok, 2 * nx * WINDOW),
                pltpu.VMEM((2 * steps, 4, tok, LANES), F32), pltpu.VMEM((2 * steps, 4, tok, LANES), F32), pltpu.VMEM((2, 4, 2 * top, tok), F32),
                vmem(local, width, ff), vmem(local, width, ff), vmem(local, ff, width),
                dma((tok // BLOCK,)), dma((tok // BLOCK,)), dma((5,)), dma((3, local)), dma,
                dma((group,)), dma((group,)), dma((128,)), dma((128,)), dma((64,)), dma((64,)), dma((8,)), dma((8,)),
                dma((16 * steps,)), dma((16 * steps,)), dma((8 * steps,)), dma((8 * steps,)),
            ],
            compiler_params=pltpu.CompilerParams(vmem_limit_bytes=67043328, collective_id=0, has_side_effects=True),
            name='step',
        )(hidden, k_cache, v_cache, lengths, w_query, w_key, w_value, w_out, w_router, mine, w_gate, w_up, w_down)

    cache_spec = P(None, BATCH_AXES, None, None, None)
    expert_spec = P(None, GROUP_AXES, None, None)
    in_specs = (P(BATCH_AXES, None), cache_spec, cache_spec, P(BATCH_AXES), P(), P(), P(), P(), P(), P(None, BATCH_AXES, None), expert_spec, expert_spec, expert_spec)
    return jax.shard_map(device_step, mesh=mesh, in_specs=in_specs, out_specs=P(BATCH_AXES, None), check_vma=False)
```
